32 devices in a mesh: gx: 2 (over x), gy: 4 (over z), gz: 4 (over y, core).
Axes of the slice: x: 2, y: 2, z: 4, core: 2. Of those that a mesh axis runs over, the one named last changes fastest.
Arguments:
- right_side: float32 [128, 256, 1024], P('gx', 'gy', 'gz'), may hold values from -5 to 7
- initial_guess: float32 [128, 256, 1024], P('gx', 'gy', 'gz'), may hold values from -5 to 7
Outputs:
- solution: float32 [128, 256, 1024], P('gx', 'gy', 'gz')
The draws below stay inside these ranges and needn't reach their ends.
All inputs are finite; a program needn't handle non-finite values.
Results may differ from the reference program's by a relative error of at most 0.000028.
Values sent between devices are 32-bit elements; how exact they have to be, the bound alone decides.
A program may use at most 128 MiB of HBM per device.

```python
import jax
import jax.numpy as jnp

COARSE_SWEEPS = 6
NX = 128
NY = 256
NZ = 1024


def ramp_field(key, rising):
    noise = jnp.clip(jax.random.normal(key, (NX, NY, NZ), jnp.float32), -5.0, 5.0)
    position = jnp.arange(NX, dtype=jnp.float32) / NX
    if rising:
        offset = 0.5 + position
    else:
        offset = 1.5 - position
    return noise + offset[:, None, None]


def draw_right_side(key, part):
    return ramp_field(jax.random.fold_in(key, 11), True)


def draw_initial_guess(key, part):
    return ramp_field(jax.random.fold_in(key, 23), False)


def setup_inputs(seed: int = 0) -> dict:
    streams_of = jax.random.split(jax.random.key(seed), 3)
    return {
        "right_side": draw_right_side(jax.random.fold_in(streams_of[2], 71), 0),
        "initial_guess": draw_initial_guess(jax.random.fold_in(streams_of[2], 71), 0),
    }


relax_weight = 0.8


def neighbours(values):
    total = jnp.roll(values, -1, 0) + jnp.roll(values, 1, 0)
    total = total + jnp.roll(values, -1, 1) + jnp.roll(values, 1, 1)
    total = total + jnp.roll(values, -1, 2) + jnp.roll(values, 1, 2)
    return total


def relax_step(centre, beside, source, level_scale):
    return centre + relax_weight * (source / (6.0 * level_scale) - centre + beside / 6.0)


def defect_of(centre, beside, source, level_scale):
    return source - level_scale * (6.0 * centre - beside)


def restrict_grid(values):
    for along in range(3):
        count_half = values.shape[along] // 2
        on_points = jax.lax.slice_in_dim(values, 0, 2 * count_half, 2, along)
        between = jax.lax.slice_in_dim(values, 1, 2 * count_half, 2, along)
        lower_side = jnp.roll(between, 1, along)
        values = 0.25 * lower_side + 0.5 * on_points + 0.25 * between
    return values


def prolong_grid(values):
    for along in range(3):
        between = 0.5 * (values + jnp.roll(values, -1, along))
        stacked = jnp.stack([values, between], along + 1)
        new_shape = list(values.shape)
        new_shape[along] = 2 * new_shape[along]
        values = stacked.reshape(new_shape)
    return values


def smoothed(approx, source, level_scale):
    return relax_step(approx, neighbours(approx), source, level_scale)


def multigrid_cycle(approx, source, grid_level):
    level_scale = 0.25 ** grid_level
    if grid_level == 2:
        approx = smoothed(jnp.zeros_like(source), source, level_scale)
        for sweep_index in range(COARSE_SWEEPS - 1):
            approx = smoothed(approx, source, level_scale)
        return approx
    approx = smoothed(smoothed(approx, source, level_scale), source, level_scale)
    defect_field = defect_of(approx, neighbours(approx), source, level_scale)
    coarse_source = restrict_grid(defect_field)
    correction = multigrid_cycle(jnp.zeros_like(coarse_source), coarse_source, grid_level + 1)
    approx = approx + prolong_grid(correction)
    return smoothed(smoothed(approx, source, level_scale), source, level_scale)


def reference(right_side, initial_guess):
    cell_count = NX * NY * NZ
    source = right_side - jnp.sum(right_side) / cell_count
    approx = initial_guess - jnp.sum(initial_guess) / cell_count
    return multigrid_cycle(approx, source, 0)
```

```python
import functools
import itertools

import jax
import jax.numpy as jnp
from jax import lax
from jax.experimental import pallas as pl
from jax.experimental.pallas import tpu as pltpu
from jax.sharding import PartitionSpec as P

COARSE_SWEEPS = 6
LANES = 128
AXES = ("gx", "gy", "gz")
relax_weight = 0.8
W = relax_weight / 6.0

HALO1 = (3, 4)
HALO2 = (COARSE_SWEEPS, COARSE_SWEEPS + 1)


def dot_exact(a, w):
    hi = a.astype(jnp.bfloat16)
    rest = a - hi.astype(jnp.float32)
    mid = rest.astype(jnp.bfloat16)
    low = (rest - mid.astype(jnp.float32)).astype(jnp.bfloat16)
    dot = functools.partial(jnp.dot, preferred_element_type=jnp.float32)
    return dot(hi, w) + (dot(mid, w) + dot(low, w))


def iotas(shape):
    return (
        lax.broadcasted_iota(jnp.int32, shape, 0),
        lax.broadcasted_iota(jnp.int32, shape, 1),
    )


def restrict_matrix(rows, cols, count, wrap=None, step=1):
    r, c = iotas((rows, cols))
    d = jnp.abs(r - 2 * step * c)
    w = jnp.where(d == 0, 0.5, 0.0) + jnp.where(d == step, 0.25, 0.0)
    w = jnp.where((c < count) & (r < 2 * step * count), w, 0.0)
    if wrap is not None:
        w = w + jnp.where((r == wrap) & (c == 0), 0.25, 0.0)
    return w.astype(jnp.bfloat16)


def prolong_matrix(rows, cols, fine, wrapped):
    r, c = iotas((rows, cols))
    if wrapped:
        r = jnp.where(r < 3 * rows // 4, r, r - rows)
        c = jnp.where(c < 3 * cols // 4, c, c - cols)
    d = jnp.abs(c - 2 * r)
    w = jnp.where(d == 0, 1.0, 0.0) + jnp.where(d == 1, 0.5, 0.0)
    return w.astype(jnp.bfloat16)


def turn(by):
    return by % LANES if isinstance(by, int) else lax.rem(by, LANES)


def extended(dims):
    (x1, y1, _), (x2, y2, _) = dims[1], dims[2]
    up = lambda n: -(-n // 8) * 8
    return (
        None,
        (x1 + sum(HALO1), up(y1 + sum(HALO1)), 2),
        (x2 + sum(HALO2), up(y2 + sum(HALO2)), 1),
    )


def buffers(dims, counts):
    (x, y, z), (x1, y1, _), (x2, y2, _) = dims
    ext = extended(dims)
    out = {}
    out["u"] = (x, y, z)
    out["f"] = (x, y, z)
    out["A0"] = (x + 1, y + 8, z)
    out["B0"] = (x, y, z)
    out["yp"] = (2, 2, x, z)
    out["zp"] = (2, y, LANES)
    out["zh"] = (y, LANES)
    out["hx"] = (5, 2, y, z)
    out["hy"] = (5, 2, x, z)
    out["hz"] = (5, 2, y, LANES)
    out["rz"] = (y + 8, LANES)
    out["rw"] = (y + 8, LANES)
    out["m"] = (y + 8, LANES)
    out["n"] = (y // 2, LANES)
    out["S"] = (4, z // LANES, y + 8, LANES)
    out["T0"] = (x1, y1, z)
    out["T1"] = (x2, y2, ext[1][2] * LANES)
    for l, n in ((1, (x1, y1)), (2, (x2, y2))):
        ex, ey, tiles = ext[l]
        for name in "GAB":
            out[f"{name}{l}"] = (ex, ey, tiles * LANES)
        out[f"zp{l}"] = (2, n[1], LANES)
        out[f"hz{l}"] = (2, 4, ey, LANES)
    out["Q1"] = (ext[2][0], ext[2][1], 2 * LANES)
    out["V1"] = (ext[2][0], 2, 2 * ext[2][1], LANES)
    out["Q0"] = (x1 + 1, ext[1][1], z)
    out["V0"] = (x1 + 1, z // LANES, y, LANES)
    out["stats"] = (3, 2, 8, LANES)
    for a in range(3):
        out[f"sums{a}"] = (counts[a], 2, 8, LANES)
    return {k: pltpu.VMEM(v, jnp.float32) for k, v in out.items()}


def kernel(dims, counts, names, cells, u_far, f_far, out, *scratch):
    b = dict(zip(names, scratch[:-3]))
    send_sem, recv_sem, load_sem = scratch[-3:]
    u, f, a0, b0 = b["u"], b["f"], b["A0"], b["B0"]
    load_u = pltpu.make_async_copy(u_far, u, load_sem.at[0])
    load_f = pltpu.make_async_copy(f_far, f, load_sem.at[1])
    load_u.start()
    load_f.start()
    here = {a: lax.axis_index(a) for a in AXES}
    serial = itertools.count()
    ext = extended(dims)
    x0, y0, z0 = dims[0]
    x1, y1, z1 = dims[1]
    x2, y2, z2 = dims[2]
    nb0, nt0 = y0 // 8, z0 // LANES
    assert 2 * x0 == LANES and z1 == LANES and 2 * z2 == LANES
    assert nt0 == 2 and y2 % 8 == 0

    def device(offset):
        return tuple(lax.rem(here[a] + (o % n), n) for a, o, n in zip(AXES, offset, counts))

    def copy(src, dst, offset):
        k = next(serial)
        c = pltpu.make_async_remote_copy(
            src_ref=src,
            dst_ref=dst,
            send_sem=send_sem.at[k],
            recv_sem=recv_sem.at[k],
            device_id=device(offset),
            device_id_type=pl.DeviceIdType.MESH,
        )
        c.start()
        return c

    def wait(copies):
        with jax.named_scope("wait"):
            for c in copies:
                c.wait()

    around = [o for o in itertools.product((-1, 0, 1), repeat=3) if any(o)]
    offsets = list(around)
    for a in range(3):
        for j in range(2, counts[a] - 1):
            offsets.append(tuple(j if i == a else 0 for i in range(3)))
    barrier = pltpu.get_barrier_semaphore()
    for o in offsets:
        pl.semaphore_signal(
            barrier, inc=1, device_id=device(o), device_id_type=pl.DeviceIdType.MESH
        )

    row8 = lax.broadcasted_iota(jnp.int32, (8, LANES), 0)
    lane8 = lax.broadcasted_iota(jnp.int32, (8, LANES), 1)
    zero8 = jnp.zeros((8, LANES), jnp.float32)

    def tile(k, t):
        return pl.ds(8 * k, 8), pl.ds(LANES * t, LANES)

    def at(i, k, t):
        return (i,) + tile(k, t)

    def groups(lo, hi, size, body):
        steps = (hi - lo) // size

        def step(p, _):
            body(lo + size * p, size)
            return 0

        if steps > 1:
            lax.fori_loop(0, steps, step, 0)
        elif steps:
            body(lo, size)
        if (hi - lo) % size:
            body(lo + size * steps, (hi - lo) % size)

    def stencil(mode, l, src, g, i, near, nb, nt, wrap, shift=None):
        scale = 0.25**l
        c = [[src[at(i, k, t)] for t in range(nt)] for k in range(nb)]
        up = [[pltpu.roll(v, 1, 0) for v in p] for p in c]
        down = [[pltpu.roll(v, 7, 0) for v in p] for p in c]
        new = []
        for k in range(nb):
            left = [pltpu.roll(v, 1, 1) for v in c[k]]
            right = [pltpu.roll(v, LANES - 1, 1) for v in c[k]]
            line = []
            for t in range(nt):
                v = c[k][t]
                above = up[k - 1][t] if k or wrap else 0.0
                below = down[(k + 1) % nb][t] if k < nb - 1 or wrap else 0.0
                s = jnp.where(row8 == 0, above, up[k][t])
                s = s + jnp.where(row8 == 7, below, down[k][t])
                if wrap and nt == 1:
                    s = s + left[t] + right[t]
                else:
                    before = left[t - 1] if t or wrap else 0.0
                    after = right[(t + 1) % nt] if t < nt - 1 or wrap else 0.0
                    s = s + jnp.where(lane8 == 0, before, left[t])
                    s = s + jnp.where(lane8 == LANES - 1, after, right[t])
                for j in near:
                    s = s + src[at(j, k, t)]
                if mode == "first":
                    z = W / scale
                    value = (W * z) * s + (W * (1.5 * z + 1.0 / scale)) * v
                elif mode == "defect":
                    value = s - 6.0 * v
                    value = g[at(i, k, t)] + (value if l == 0 else scale * value)
                else:
                    gv = g[at(i, k, t)]
                    value = s + 1.5 * v
                    value = value + (gv if l == 0 else (1.0 / scale) * gv)
                    value = W * value
                    if shift is not None:
                        value = value - shift
                line.append(value)
            new.append(line)
        return new

    def put(dst, i, new):
        for k, line in enumerate(new):
            for t, value in enumerate(line):
                dst[at(i, k, t)] = value

    zh = b["zh"]
    last = LANES - 1

    def pack_z(zp, i, ref, blocks=range(nb0)):
        moved = []
        for k in blocks:
            both = jnp.where(lane8 == last, ref[at(i, k, nt0 - 1)], ref[at(i, k, 0)])
            moved.append(pltpu.roll(both, turn(2 * i + 1), 1))
        mask = (lane8 == 2 * i) | (lane8 == 2 * i + 1)
        for k, v in zip(blocks, moved):
            pltpu.store(zp.at[pl.ds(8 * k, 8), :], v, mask=mask)

    def pack_rows(yp, i, new):
        for side, (k, r) in enumerate(((0, 0), (nb0 - 1, 7))):
            yp[side, pl.ds(i, 1), :] = jnp.concatenate([v[r : r + 1] for v in new[k]], 1)

    def exchange(r, src, yl, yh):
        hx, hy, hz = b["hx"].at[r], b["hy"].at[r], b["hz"].at[r]
        zp = b["zp"].at[r % 2]
        rows = pl.ds(0, y0)

        def send_x(ref=None):
            ref = src if ref is None else ref
            return [
                copy(ref.at[x0 - 1, rows], hx.at[0], (1, 0, 0)),
                copy(ref.at[0, rows], hx.at[1], (-1, 0, 0)),
            ]

        def send_y():
            return [
                copy(yh, hy.at[0], (0, 1, 0)),
                copy(yl, hy.at[1], (0, -1, 0)),
            ]

        def send_z():
            return [
                copy(zp, hz.at[0], (0, 0, 1)),
                copy(zp, hz.at[1], (0, 0, -1)),
            ]

        return send_x, send_y, send_z

    def defect_exchange(r, d):
        rz, rw = b["rz"], b["rw"]
        yp, zp = b["yp"].at[r % 2], b["zp"].at[r % 2]

        def send_x():
            return [copy(d.at[x0 - 1, pl.ds(0, y0)], d.at[x0, pl.ds(0, y0)], (1, 0, 0))]

        def send_y():
            return [
                copy(yp.at[1, x0 - 1], d.at[x0, y0 + 7], (1, 1, 0)),
                copy(yp.at[1], d.at[pl.ds(0, x0), y0 + 7], (0, 1, 0)),
            ]

        def send_z():
            end, all_rows = zp.at[pl.ds(y0 - 1, 1)], pl.ds(8, y0)
            return [
                copy(end, rw.at[pl.ds(7, 1)], (1, 1, 1)),
                copy(zp, rw.at[all_rows], (1, 0, 1)),
                copy(end, rz.at[pl.ds(7, 1)], (0, 1, 1)),
                copy(zp, rz.at[all_rows], (0, 0, 1)),
            ]

        return send_x, send_y, send_z

    def sweep(r, moving, src, dst, onward=None, mode="relax", shift=None):
        hx, hy, hz = b["hx"].at[r], b["hy"].at[r], b["hz"].at[r]
        yp, zp = b["yp"].at[(r + 1) % 2], b["zp"].at[(r + 1) % 2]
        gain = 1.0 if mode == "defect" else W
        packed = onward is not None

        def plane(i, near):
            new = stencil(mode, 0, src, f, i, near, nb0, nt0, False, shift)
            put(dst, i, new)
            if packed:
                pack_rows(yp, i, new)

        def pair(p, _):
            i = 1 + 2 * p
            plane(i, (i - 1, i + 1))
            plane(i + 1, (i, i + 2))
            if packed:
                pack_z(zp, i - 2, dst)
                pack_z(zp, i - 1, dst)
            return 0

        with jax.named_scope("inner"):
            plane(0, (1,))
            plane(x0 - 1, (x0 - 2,))
            plane(1, (0, 2))
            plane(2, (1, 3))
            lax.fori_loop(1, (x0 - 2) // 2, pair, 0)
            if packed:
                pack_z(zp, x0 - 3, dst)
                pack_z(zp, x0 - 2, dst)
        wait(moving)
        odd = lane8 % 2 == 1
        for k in range(nb0):
            rows = pl.ds(8 * k, 8)
            before = pltpu.roll(hz[0, rows, :], 1, 1)
            after = pltpu.roll(hz[1, rows, :], LANES - 1, 1)
            zh[rows, :] = gain * jnp.where(odd, before, after)

        def fix(i, size, beyond=None):
            done = []
            for p in range(i, i + size) if isinstance(i, int) else [i + q for q in range(size)]:
                edges = [gain * hy[s, pl.ds(p, 1), :] for s in range(2)]
                for k in range(nb0):
                    halo = pltpu.roll(zh[pl.ds(8 * k, 8), :], turn(2 * LANES - 2 * p - 1), 1)
                    inside = 0 < k < nb0 - 1 and beyond is None
                    for t in (0, nt0 - 1) if inside else range(nt0):
                        v = dst[at(p, k, t)]
                        if beyond is not None:
                            v = v + gain * beyond[tile(k, t)]
                        for s, kk, rr in ((0, 0, 0), (1, nb0 - 1, 7)):
                            if k == kk:
                                edge = edges[s][:, LANES * t : LANES * t + LANES]
                                v = v + jnp.where(row8 == rr, edge, 0.0)
                        if t == 0:
                            v = v + jnp.where(lane8 == 0, halo, 0.0)
                        if t == nt0 - 1:
                            v = v + jnp.where(lane8 == last, halo, 0.0)
                        done.append((at(p, k, t), v))
            for where, v in done:
                dst[where] = v

        with jax.named_scope("ends"):
            fix(0, 1, hx.at[0])
            fix(x0 - 1, 1, hx.at[1])
        if not packed:
            with jax.named_scope("fix"):
                groups(1, x0 - 1, 4, fix)
            return []
        started = onward[0]()
        with jax.named_scope("yface"):
            for side, r0 in ((0, 0), (1, y0 - 1)):
                line = jnp.broadcast_to(zh[pl.ds(r0, 1), :], (8, LANES))
                for j in range(x0 // 8):
                    slot = 2 * (8 * j + row8)
                    low = jnp.sum(jnp.where(lane8 == slot + 1, line, 0.0), 1, keepdims=True)
                    high = jnp.sum(jnp.where(lane8 == slot, line, 0.0), 1, keepdims=True)
                    for t in range(nt0):
                        rows = (side,) + tile(j, t)
                        v = yp[rows] + gain * hy[rows]
                        if t == 0:
                            v = v + jnp.where(lane8 == 0, low, 0.0)
                        if t == nt0 - 1:
                            v = v + jnp.where(lane8 == last, high, 0.0)
                        yp[rows] = v
                for i in (0, x0 - 1):
                    yp[side, pl.ds(i, 1), :] = dst[i, pl.ds(r0, 1), :]
        started = started + onward[1]()
        with jax.named_scope("zface"):
            for k in range(nb0):
                v = zp[pl.ds(8 * k, 8), :] + zh[pl.ds(8 * k, 8), :]
                for side, kk, rr in ((0, 0, 0), (1, nb0 - 1, 7)):
                    if k == kk:
                        total = zero8
                        for j in range(x0 // 8):
                            slot = 2 * (8 * j + row8)
                            low = hy[(side,) + tile(j, 0)][:, :1]
                            high = hy[(side,) + tile(j, nt0 - 1)][:, last:]
                            total = total + jnp.where(lane8 == slot + 1, low, 0.0)
                            total = total + jnp.where(lane8 == slot, high, 0.0)
                        total = gain * jnp.sum(total, 0, keepdims=True)
                        v = v + jnp.where(row8 == rr, total, 0.0)
                zp[pl.ds(8 * k, 8), :] = v
            pack_z(zp, 0, dst)
            pack_z(zp, x0 - 1, dst)
        started = started + onward[2]()
        with jax.named_scope("fix"):
            groups(1, x0 - 1, 4, fix)
        return started

    def restrict_xy(d, before, j, u_slot, nb, top, nt, dst):
        s = b["S"].at[u_slot]
        low = 2 * j - 1 if before is None else before
        for t in range(nt):
            for q, k in enumerate((top,) + tuple(range(nb))):
                v = 0.25 * (d[at(low, k, t)] + d[at(2 * j + 1, k, t)])
                s[t, pl.ds(8 * q, 8), :] = v + 0.5 * d[at(2 * j, k, t)]
        n = nb * 4
        for t in range(nt):
            v = 0.25 * (s[t, pl.ds(7, n, stride=2), :] + s[t, pl.ds(9, n, stride=2), :])
            dst[j, :, pl.ds(LANES * t, LANES)] = v + 0.5 * s[t, pl.ds(8, n, stride=2), :]

    def restrict_planes(d, before, nb, top, nt, dst, count):
        restrict_xy(d, before, 0, 0, nb, top, nt, dst)
        for j in range(1, 4):
            restrict_xy(d, None, j, j, nb, top, nt, dst)

        def some(p, _):
            for q in range(4):
                restrict_xy(d, None, 4 * p + q, q, nb, top, nt, dst)
            return 0

        lax.fori_loop(1, count // 4, some, 0)

    def multiply(src, dst, w, first, count, chunk, rows, cols):
        zs = src.shape[2]

        def step(k, _):
            i = first + k * chunk if not isinstance(k, int) else first
            v = src[pl.ds(i, chunk), pl.ds(0, rows), :].reshape(chunk * rows, zs)
            v = dot_exact(v, w).reshape(chunk, rows, cols)
            dst[pl.ds(i, chunk), pl.ds(0, rows), pl.ds(0, cols)] = v
            return 0

        if count == chunk:
            step(0, 0)
        else:
            lax.fori_loop(0, count // chunk, step, 0)

    def region(o, n, size, depth):
        lo, hi = depth
        if o == 1:
            return pl.ds(n - lo, lo), pl.ds(size - lo, lo)
        if o == -1:
            return pl.ds(0, hi), pl.ds(n, hi)
        return pl.ds(0, n), pl.ds(0, n)

    def halo_send(l, depth, beside):
        g, zpl, hzl = b[f"G{l}"], b[f"zp{l}"], b[f"hz{l}"]
        nx, ny, _ = dims[l]
        ex, ey, _ = ext[l]
        started = []
        lanes = pl.ds(0, LANES)
        for o in sorted(around, key=lambda v: -sum(map(abs, v))):
            if (o[2] != 0) == beside:
                continue
            sx, dx = region(o[0], nx, ex, depth)
            sy, dy = region(o[1], ny, ey, depth)
            if beside:
                started.append(copy(g.at[sx, sy, lanes], g.at[dx, dy, lanes], o))
            else:
                side = 0 if o[2] == 1 else 1
                half = {0: (0, 2), 1: (1, 1), -1: (0, 1)}[o[0]]
                slot = {0: 0, 1: 2, -1: 3}[o[0]]
                source = zpl.at[pl.ds(*half), sy]
                started.append(copy(source, hzl.at[side, pl.ds(slot, half[1]), dy], o))
        return started

    def halo_pack(l, depth):
        g, zpl = b[f"G{l}"], b[f"zp{l}"]
        nx, ny, nz = dims[l]
        lo, hi = depth
        width, per = lo + hi, nx // 2
        for half in range(2):
            total = [zero8] * (ny // 8)
            for p in range(per):
                first = width * p
                mask = (lane8 >= first) & (lane8 < first + width)
                for k in range(ny // 8):
                    v = g[at(half * per + p, k, 0)]
                    if nz < LANES:
                        v = jnp.where(lane8 < LANES - nz, v, pltpu.roll(v, LANES - nz, 1))
                    v = pltpu.roll(v, first + lo, 1)
                    total[k] = jnp.where(mask, v, total[k])
            for k in range(ny // 8):
                zpl[half, pl.ds(8 * k, 8), :] = total[k]

    def halo_unpack(l, depth):
        g, hzl = b[f"G{l}"], b[f"hz{l}"]
        nx, ny, nz = dims[l]
        ex, ey, tiles = ext[l]
        lo, hi = depth
        width, per = lo + hi, nx // 2
        left = lane8 < lo
        for p in range(1, per):
            left = left | ((lane8 >= width * p) & (lane8 < width * p + lo))
        for slot in range(4):
            for k in range(ey // 8):
                rows = pl.ds(8 * k, 8)
                hzl[0, slot, rows, :] = jnp.where(left, hzl[0, slot, rows, :], hzl[1, slot, rows, :])
        for e in range(ex):
            if e < nx:
                slot, p = e // per, e % per
            elif e < nx + hi:
                slot, p = 3, e - nx
            else:
                slot, p = 2, (nx - ex + e) % per
            back = LANES - (width * p + lo)
            for k in range(ey // 8):
                v = hzl[0, slot, pl.ds(8 * k, 8), :]
                moved = pltpu.roll(v, back % LANES, 1)
                if nz < LANES:
                    high = pltpu.roll(v, (back + nz) % LANES, 1)
                    moved = jnp.where(lane8 < (nz + LANES) // 2, high, moved)
                    g[at(e, k, 0)] = jnp.where(lane8 < nz, g[at(e, k, 0)], moved)
                else:
                    g[at(e, k, tiles - 1)] = moved

    def ext_sweep(mode, l, src, dst, size):
        ex, ey, nt = ext[l]
        nb = ey // 8
        g = b[f"G{l}"]

        def some(i, count):
            for q in range(count):
                p = i + q
                near = ((p - 1) % ex, (p + 1) % ex) if isinstance(p, int) else (p - 1, p + 1)
                put(dst, p, stencil(mode, l, src, g, p, near, nb, nt, True))

        some(0, 1)
        groups(1, ex - 1, size, some)
        some(ex - 1, 1)

    def spread_rows(q, v, j, k, kn, t, slot_k):
        c, n = q[at(j, k, t)], q[at(j, kn, t)]
        below = jnp.where(row8 == 7, pltpu.roll(n, 7, 0), pltpu.roll(c, 7, 0))
        v[j, t, pl.ds(16 * slot_k, 8, stride=2), :] = c
        v[j, t, pl.ds(16 * slot_k + 1, 8, stride=2), :] = 0.5 * (c + below)

    st, sg = b["stats"], [b[f"sums{a}"] for a in range(3)]

    def spread_sums(a):
        return [
            copy(st.at[a], sg[a].at[j], tuple(j if i == a else 0 for i in range(3)))
            for j in range(1, counts[a])
        ]

    def gather_sums(a, copies):
        wait(copies)
        total = st[a]
        for j in range(1, counts[a]):
            total = total + sg[a][j]
        if a < 2:
            st[a + 1] = total
        return total

    def fold(ref):
        def step(p, totals):
            totals = list(totals)
            for q in range(2):
                for k in range(nb0):
                    for t in range(nt0):
                        totals[(2 * k + t) % 4] += ref[at(2 * p + q, k, t)]
            return tuple(totals)

        t = lax.fori_loop(0, x0 // 2, step, (zero8,) * 4)
        return (t[0] + t[1]) + (t[2] + t[3])

    a1, b1, g1 = b["A1"], b["B1"], b["G1"]
    a2, b2, g2 = b["A2"], b["B2"], b["G2"]

    with jax.named_scope("clear"):
        for ref in (g1, g2):
            shape = ref.shape

            def clear(i, _, ref=ref, shape=shape):
                for k in range(shape[1] // 8):
                    for t in range(shape[2] // LANES):
                        ref[at(i, k, t)] = zero8
                return 0

            lax.fori_loop(0, shape[0], clear, 0)
        for l in (1, 2):
            hzl = b[f"hz{l}"]
            for side in range(2):
                for slot in range(4):
                    for k in range(ext[l][1] // 8):
                        hzl[side, slot, pl.ds(8 * k, 8), :] = zero8
    with jax.named_scope("barrier"):
        pl.semaphore_wait(barrier, len(offsets))
    with jax.named_scope("loadu"):
        load_u.wait()
    send_x, send_y, send_z = exchange(0, u, u.at[:, 0, :], u.at[:, y0 - 1, :])
    moving = send_x() + send_y()
    with jax.named_scope("packu"):

        def pack_some(i, count):
            for q in range(count):
                pack_z(b["zp"].at[0], i + q, u)

        groups(0, x0, 8, pack_some)
    moving = moving + send_z()
    with jax.named_scope("sums"):
        st[0, 0] = fold(u)
        load_f.wait()
        st[0, 1] = fold(f)
    sums = spread_sums(0)
    rows = [(b["yp"].at[r % 2, 0], b["yp"].at[r % 2, 1]) for r in range(5)]
    moving = sweep(0, moving, u, a0, exchange(1, a0, *rows[1]))
    gather_sums(0, sums)
    sums = spread_sums(1)
    moving = sweep(1, moving, a0, b0, exchange(2, b0, *rows[2]))
    gather_sums(1, sums)
    sums = spread_sums(2)
    moving = sweep(2, moving, b0, a0, defect_exchange(3, a0), mode="defect")
    total = gather_sums(2, sums)
    mean_u = jnp.sum(total[0]) * (1.0 / cells)
    mean_f = jnp.sum(total[1]) * (1.0 / cells)
    wait(moving)

    with jax.named_scope("restrict0"):
        lane = lax.broadcasted_iota(jnp.int32, (y0 + 8, LANES), 1)
        moved = pltpu.roll(b["rw"][...], 1, 1)
        rim = jnp.where(lane == last, moved, b["rz"][...])
        b["m"][...] = dot_exact(rim, restrict_matrix(LANES, LANES, x1, last, 2))
        m = b["m"]
        v = 0.25 * (m[pl.ds(7, y1, stride=2), :] + m[pl.ds(9, y1, stride=2), :])
        b["n"][...] = 0.25 * (v + 0.5 * m[pl.ds(8, y1, stride=2), :])
        restrict_planes(a0, x0, nb0, nb0, nt0, b["T0"], x1)
        w = restrict_matrix(z0, LANES, z1)
        multiply(b["T0"], g1, w, 0, x1, 8, y1, LANES)

        def finish(i, count):
            for q in range(count):
                for k in range(y1 // 8):
                    col = pltpu.roll(b["n"][pl.ds(8 * k, 8), :], turn(2 * LANES - (i + q)), 1)
                    v = g1[at(i + q, k, 0)] + jnp.where(lane8 == 0, col, 0.0)
                    g1[at(i + q, k, 0)] = v - mean_f

        groups(0, x1, 8, finish)
    moving = halo_send(1, HALO1, True)
    with jax.named_scope("pack1"):
        halo_pack(1, HALO1)
    moving = moving + halo_send(1, HALO1, False)
    wait(moving)
    with jax.named_scope("unpack1"):
        halo_unpack(1, HALO1)
    with jax.named_scope("first1"):
        ext_sweep("first", 1, g1, b1, 6)
    with jax.named_scope("defect1"):
        ext_sweep("defect", 1, b1, a1, 6)
    with jax.named_scope("restrict1"):
        e1 = ext[1]
        restrict_planes(a1, e1[0] - 1, y1 // 8, e1[1] // 8 - 1, e1[2], b["T1"], x2)
        w = restrict_matrix(2 * LANES, LANES, z2, 2 * LANES - 1)
        multiply(b["T1"], g2, w, 0, x2, x2, y2, LANES)
    moving = halo_send(2, HALO2, True)
    with jax.named_scope("pack2"):
        halo_pack(2, HALO2)
    moving = moving + halo_send(2, HALO2, False)
    wait(moving)
    with jax.named_scope("unpack2"):
        halo_unpack(2, HALO2)
    with jax.named_scope("sweeps2"):
        v, w2 = a2, b2
        ext_sweep("first", 2, g2, v, 9)
        for _ in range(COARSE_SWEEPS - 2):
            ext_sweep("relax", 2, v, w2, 9)
            v, w2 = w2, v
    with jax.named_scope("prolong1"):
        e2 = ext[2]
        q1, v1 = b["Q1"], b["V1"]
        w = prolong_matrix(LANES, 2 * LANES, z1, True)
        multiply(v, q1, w, 0, x2 + 2, (x2 + 2) // 3, e2[1], 2 * LANES)
        multiply(v, q1, w, e2[0] - 1, 1, 1, e2[1], 2 * LANES)
        nb2, top1 = e2[1] // 8, e1[1] // 8 - 1
        need = -(-(y1 + 3) // 16)

        def spread1(i, count):
            for q in range(count):
                for t in range(2):
                    for k in range(need):
                        spread_rows(q1, v1, i + q, k, k + 1, t, k)
                    spread_rows(q1, v1, i + q, nb2 - 1, 0, t, nb2 - 1)

        groups(0, x2 + 2, 3, spread1)
        spread1(e2[0] - 1, 1)

        def fine1(j, k, t):
            if k < top1:
                return v1[j, t, pl.ds(8 * k, 8), :]
            high = v1[j, t, pl.ds(8 * k, 8), :]
            low = v1[j, t, pl.ds(16 * nb2 - 8, 8), :]
            return jnp.where(row8 < 4, high, low)

        def add1(j, jn, i):
            for k in range(top1 + 1):
                for t in range(2):
                    c, n = fine1(j, k, t), fine1(jn, k, t)
                    b1[at(i, k, t)] = b1[at(i, k, t)] + c
                    b1[at(i + 1, k, t)] = b1[at(i + 1, k, t)] + 0.5 * (c + n)

        def add1_some(i, count):
            for q in range(count):
                add1(i + q, i + q + 1, 2 * (i + q))

        groups(0, x2 + 1, 2, add1_some)
        for k in range(top1 + 1):
            for t in range(2):
                b1[at(x1 + 2, k, t)] = b1[at(x1 + 2, k, t)] + fine1(x2 + 1, k, t)
        add1(e2[0] - 1, 0, e1[0] - 2)
    with jax.named_scope("post1"):
        ext_sweep("relax", 1, b1, a1, 6)
        ext_sweep("relax", 1, a1, b1, 6)
    with jax.named_scope("prolong0"):
        q0, v0 = b["Q0"], b["V0"]
        w = prolong_matrix(2 * LANES, z0, z0, False)
        multiply(b1, q0, w, 0, x1 + 1, 3, e1[1], z0)

        def spread0(i, count):
            for q in range(count):
                for t in range(nt0):
                    for k in range(y1 // 8):
                        spread_rows(q0, v0, i + q, k, k + 1, t, k)

        groups(0, x1 + 1, 3, spread0)
        shift = mean_u + 2.0 * W * mean_f

        def add0(j):
            for k in range(nb0):
                for t in range(nt0):
                    c = v0[j, t, pl.ds(8 * k, 8), :] - shift
                    n = v0[j + 1, t, pl.ds(8 * k, 8), :] - shift
                    b0[at(2 * j, k, t)] = b0[at(2 * j, k, t)] + c
                    b0[at(2 * j + 1, k, t)] = b0[at(2 * j + 1, k, t)] + 0.5 * (c + n)

        def add0_some(i, count):
            for q in range(count):
                add0(i + q)

        send_x, send_y, send_z = exchange(3, b0, b0.at[:, 0, :], b0.at[:, y0 - 1, :])
        add0(0)
        add0(x1 - 1)
        moving = send_x()
        groups(1, x1 - 1, 2, add0_some)
        moving = moving + send_y()

        def pack_b0(i, count):
            for q in range(count):
                pack_z(b["zp"].at[1], i + q, b0)

        groups(0, x0, 8, pack_b0)
        moving = moving + send_z()
    moving = sweep(3, moving, b0, a0, exchange(4, a0, *rows[4]), shift=W * mean_f)
    sweep(4, moving, a0, out, shift=W * mean_f)


def solution(mesh):
    counts = tuple(mesh.shape[a] for a in AXES)

    def shards(right_side, initial_guess):
        shape = right_side.shape
        dims = tuple(tuple(n >> l for n in shape) for l in range(3))
        cells = float(right_side.size)
        for n in counts:
            cells *= n
        bufs = buffers(dims, counts)
        messages = 5 * 6 + 7 + 2 * 26 + sum(counts) - 3
        return pl.pallas_call(
            functools.partial(kernel, dims, counts, tuple(bufs), cells),
            out_shape=jax.ShapeDtypeStruct(shape, jnp.float32),
            in_specs=[pl.BlockSpec(memory_space=pl.ANY)] * 2,
            out_specs=pl.BlockSpec(memory_space=pltpu.VMEM),
            scratch_shapes=list(bufs.values())
            + [pltpu.SemaphoreType.DMA((n,)) for n in (messages, messages, 2)],
            compiler_params=pltpu.CompilerParams(
                collective_id=0, has_side_effects=True, vmem_limit_bytes=56 * 1024 * 1024
            ),
        )(initial_guess, right_side)

    placed = (P(*AXES), P(*AXES))
    return jax.shard_map(
        shards, mesh=mesh, in_specs=placed, out_specs=P(*AXES), check_vma=False
    )
```

```python
import functools
import itertools

import jax
import jax.numpy as jnp
from jax import lax
from jax.experimental import pallas as pl
from jax.experimental.pallas import tpu as pltpu
from jax.sharding import PartitionSpec as P

COARSE_SWEEPS = 6
LANES = 128
AXES = ("gx", "gy", "gz")
relax_weight = 0.8
W = relax_weight / 6.0

SWEEP_PLANES = 10
FIX_PLANES = 12

HALO1 = (3, 4)
HALO2 = (COARSE_SWEEPS, COARSE_SWEEPS + 1)


def dot_split(a, w):
    hi = a.astype(jnp.bfloat16)
    mid = (a - hi.astype(jnp.float32)).astype(jnp.bfloat16)
    dot = functools.partial(jnp.dot, preferred_element_type=jnp.float32)
    return dot(hi, w) + dot(mid, w)


def iotas(shape):
    return (
        lax.broadcasted_iota(jnp.int32, shape, 0),
        lax.broadcasted_iota(jnp.int32, shape, 1),
    )


def restrict_matrix(rows, cols, count, wrap=None, step=1):
    r, c = iotas((rows, cols))
    d = jnp.abs(r - 2 * step * c)
    w = jnp.where(d == 0, 0.5, 0.0) + jnp.where(d == step, 0.25, 0.0)
    w = jnp.where((c < count) & (r < 2 * step * count), w, 0.0)
    if wrap is not None:
        w = w + jnp.where((r == wrap) & (c == 0), 0.25, 0.0)
    return w.astype(jnp.bfloat16)


def prolong_matrix(rows, cols, fine, wrapped):
    r, c = iotas((rows, cols))
    if wrapped:
        r = jnp.where(r < 3 * rows // 4, r, r - rows)
        c = jnp.where(c < 3 * cols // 4, c, c - cols)
    d = jnp.abs(c - 2 * r)
    w = jnp.where(d == 0, 1.0, 0.0) + jnp.where(d == 1, 0.5, 0.0)
    return w.astype(jnp.bfloat16)


def turn(by):
    return by % LANES if isinstance(by, int) else lax.rem(by, LANES)


OWN = 8


def extended(dims):
    (x1, y1, _), (x2, y2, _) = dims[1], dims[2]
    up = lambda n: -(-n // 8) * 8
    return (
        None,
        (x1 + sum(HALO1), up(y1 + OWN + HALO1[1] + 9), 2, HALO1[0]),
        (x2 + sum(HALO2), up(y2 + OWN + HALO2[1] + 4), 1, HALO2[0]),
    )


def buffers(dims, counts):
    (x, y, z), (x1, y1, _), (x2, y2, _) = dims
    ext = extended(dims)
    nt = z // LANES
    out = {}
    for name in ("u", "f", "A0", "B0"):
        out[name] = (x, nt, y + 2 * OWN, LANES)
    out["D0"] = (x + 1, nt, y + OWN, LANES)
    out["yp"] = (2, 2, nt, x, LANES)
    out["zp"] = (2, y, LANES)
    out["zh"] = (y, LANES)
    out["hx"] = (5, 2, nt, y, LANES)
    out["hy"] = (5, 2, nt, x, LANES)
    out["hz"] = (5, 2, y, LANES)
    out["rz"] = (y + OWN, LANES)
    out["rw"] = (y + OWN, LANES)
    out["m"] = (y + OWN, LANES)
    out["n"] = (y // 2, LANES)
    out["S"] = (4, nt, y + OWN, LANES)
    out["T0"] = (x1, nt, y1, LANES)
    out["T1"] = (x2, 2, y2, LANES)
    for l, ny in ((1, y1), (2, y2)):
        ex, ey, tiles, _ = ext[l]
        for name in "GAB":
            out[f"{name}{l}"] = (ex, tiles, ey, LANES)
        out[f"zp{l}"] = (2, ny, LANES)
        out[f"hz{l}"] = (2, 4, ey, LANES)
    out["P2"] = (x2 // 2 + -(-HALO2[0] // 2) + -(-HALO2[1] // 2), ext[2][1], LANES)
    out["Q1"] = (ext[2][0], 2, ext[2][1], LANES)
    out["V1"] = (ext[2][0], 2, ext[1][1] + 8, LANES)
    out["Q0"] = (x1 + 1, nt, ext[1][1], LANES)
    out["V0"] = (x1 + 1, nt, y, LANES)
    out["stats"] = (3, 2, 8, LANES)
    for a in range(3):
        out[f"sums{a}"] = (counts[a], 2, 8, LANES)
    return {k: pltpu.VMEM(v, jnp.float32) for k, v in out.items()}


def kernel(dims, counts, names, cells, u_far, f_far, out, *scratch):
    b = dict(zip(names, scratch[:-3]))
    send_sem, recv_sem, load_sem = scratch[-3:]
    u, f, a0, b0, d0 = b["u"], b["f"], b["A0"], b["B0"], b["D0"]
    loads = []
    for n, (far, near) in enumerate(((u_far, u), (f_far, f))):
        for t in range(2):
            lanes = pl.ds(LANES * t, LANES)
            own = near.at[:, t, pl.ds(OWN, dims[0][1]), :]
            c = pltpu.make_async_copy(far.at[:, :, lanes], own, load_sem.at[2 * n + t])
            c.start()
            loads.append(c)
    here = {a: lax.axis_index(a) for a in AXES}
    serial = itertools.count()
    ext = extended(dims)
    x0, y0, z0 = dims[0]
    x1, y1, z1 = dims[1]
    x2, y2, z2 = dims[2]
    nb0, nt0 = y0 // 8, z0 // LANES
    assert 2 * x0 == LANES and z1 == LANES and 2 * z2 == LANES
    assert nt0 == 2 and y2 % 8 == 0

    def device(offset):
        return tuple(lax.rem(here[a] + (o % n), n) for a, o, n in zip(AXES, offset, counts))

    def copy(src, dst, offset):
        k = next(serial)
        c = pltpu.make_async_remote_copy(
            src_ref=src,
            dst_ref=dst,
            send_sem=send_sem.at[k],
            recv_sem=recv_sem.at[k],
            device_id=device(offset),
            device_id_type=pl.DeviceIdType.MESH,
        )
        c.start()
        return c

    def wait(copies):
        with jax.named_scope("wait"):
            for c in copies:
                c.wait()

    around = [o for o in itertools.product((-1, 0, 1), repeat=3) if any(o)]
    offsets = list(around)
    for a in range(3):
        for j in range(2, counts[a] - 1):
            offsets.append(tuple(j if i == a else 0 for i in range(3)))
    barrier = pltpu.get_barrier_semaphore()
    for o in offsets:
        pl.semaphore_signal(
            barrier, inc=1, device_id=device(o), device_id_type=pl.DeviceIdType.MESH
        )

    row8 = lax.broadcasted_iota(jnp.int32, (8, LANES), 0)
    lane8 = lax.broadcasted_iota(jnp.int32, (8, LANES), 1)
    zero8 = jnp.zeros((8, LANES), jnp.float32)

    def at(i, k, t, first=OWN):
        return i, t, pl.ds(first + 8 * k, 8), slice(None)

    def groups(lo, hi, size, body):
        steps = (hi - lo) // size

        def step(p, _):
            body(lo + size * p, size)
            return 0

        if steps > 1:
            lax.fori_loop(0, steps, step, 0)
        elif steps:
            body(lo, size)
        if (hi - lo) % size:
            body(lo + size * steps, (hi - lo) % size)

    def lanes_of(rows):
        return lax.broadcasted_iota(jnp.int32, (rows, LANES), 1)

    def stencil(mode, l, src, g, i, near, first, rows, nt, z_wrap, shift=None):
        scale = 0.25**l
        lane = lanes_of(rows)
        here, above, below = (pl.ds(first + d, rows) for d in (0, -1, 1))
        c = [src[i, t, here, :] for t in range(nt)]
        left = [pltpu.roll(v, 1, 1) for v in c]
        right = [pltpu.roll(v, LANES - 1, 1) for v in c]
        new = []
        for t in range(nt):
            v = c[t]
            s = src[i, t, above, :] + src[i, t, below, :]
            for j in near:
                s = s + src[j, t, here, :]
            if z_wrap and nt == 1:
                s = s + (left[t] + right[t])
            else:
                before = left[t - 1] if t or z_wrap else 0.0
                after = right[(t + 1) % nt] if t < nt - 1 or z_wrap else 0.0
                z = jnp.where(lane == 0, before, left[t])
                s = s + (z + jnp.where(lane == LANES - 1, after, right[t]))
            if mode == "first":
                z = W / scale
                value = (W * z) * s + (W * (1.5 * z + 1.0 / scale)) * v
            elif mode == "defect":
                value = s - 6.0 * v
                value = g[i, t, here, :] + (value if l == 0 else scale * value)
            else:
                gv = g[i, t, here, :]
                value = s + 1.5 * v
                value = W * (value + (gv if l == 0 else (1.0 / scale) * gv))
                if shift is not None:
                    value = value - shift
            new.append(value)
        return new

    zh = b["zh"]
    last = LANES - 1

    def pack_z(zp, i, ref):
        lane = lanes_of(y0)
        both = jnp.where(lane == last, ref[i, nt0 - 1, own0, :], ref[i, 0, own0, :])
        moved = pltpu.roll(both, turn(2 * i + 1), 1)
        pltpu.store(zp, moved, mask=(lane == 2 * i) | (lane == 2 * i + 1))

    def pack_rows(yp, i, new):
        for side, r in ((0, 0), (1, y0 - 1)):
            for t in range(nt0):
                yp[side, t, pl.ds(i, 1), :] = new[t][r : r + 1]

    own0 = pl.ds(OWN, y0)

    def exchange(r, src, faces=None):
        hx, hy, hz = b["hx"].at[r], b["hy"].at[r], b["hz"].at[r]
        zp = b["zp"].at[r % 2]

        def send_x():
            return [
                copy(src.at[x0 - 1, :, own0], hx.at[0], (1, 0, 0)),
                copy(src.at[0, :, own0], hx.at[1], (-1, 0, 0)),
            ]

        def send_y():
            if faces is not None:
                return [
                    copy(faces.at[1], hy.at[0], (0, 1, 0)),
                    copy(faces.at[0], hy.at[1], (0, -1, 0)),
                ]
            started = []
            for t in range(nt0):
                started.append(copy(src.at[:, t, OWN + y0 - 1], hy.at[0, t], (0, 1, 0)))
                started.append(copy(src.at[:, t, OWN], hy.at[1, t], (0, -1, 0)))
            return started

        def send_z():
            return [
                copy(zp, hz.at[0], (0, 0, 1)),
                copy(zp, hz.at[1], (0, 0, -1)),
            ]

        return send_x, send_y, send_z

    def defect_exchange(r, d):
        rz, rw = b["rz"], b["rw"]
        yp, zp = b["yp"].at[r % 2], b["zp"].at[r % 2]

        def send_x():
            return [copy(d.at[x0 - 1, :, own0], d.at[x0, :, own0], (1, 0, 0))]

        def send_y():
            started = []
            for t in range(nt0):
                started.append(copy(yp.at[1, t, x0 - 1], d.at[x0, t, OWN - 1], (1, 1, 0)))
                started.append(copy(yp.at[1, t], d.at[pl.ds(0, x0), t, OWN - 1], (0, 1, 0)))
            return started

        def send_z():
            end, before = zp.at[pl.ds(y0 - 1, 1)], pl.ds(OWN - 1, 1)
            return [
                copy(end, rw.at[before], (1, 1, 1)),
                copy(zp, rw.at[own0], (1, 0, 1)),
                copy(end, rz.at[before], (0, 1, 1)),
                copy(zp, rz.at[own0], (0, 0, 1)),
            ]

        return send_x, send_y, send_z

    def sweep(r, moving, src, dst, onward=None, mode="relax", shift=None):
        hx, hy, hz = b["hx"].at[r], b["hy"].at[r], b["hz"].at[r]
        yp, zp = b["yp"].at[(r + 1) % 2], b["zp"].at[(r + 1) % 2]
        gain = 1.0 if mode == "defect" else W
        packed = onward is not None

        def plane(i, near):
            new = stencil(mode, 0, src, f, i, near, OWN, y0, nt0, False, shift)
            for t, value in enumerate(new):
                if packed:
                    dst[i, t, own0, :] = value
                else:
                    dst[i, :, pl.ds(LANES * t, LANES)] = value
            if packed:
                pack_rows(yp, i, new)

        def some(i, count):
            for q in range(count):
                plane(i + q, (i + q - 1, i + q + 1))
            if packed:
                for q in range(count):
                    pack_z(zp, i + q - 2, dst)

        with jax.named_scope("inner"):
            plane(0, (1,))
            plane(x0 - 1, (x0 - 2,))
            plane(1, (0, 2))
            plane(2, (1, 3))
            groups(3, x0 - 1, SWEEP_PLANES, some)
            if packed:
                pack_z(zp, x0 - 3, dst)
                pack_z(zp, x0 - 2, dst)
        wait(moving)
        odd = lane8 % 2 == 1
        for k in range(nb0):
            rows = pl.ds(8 * k, 8)
            before = pltpu.roll(hz[0, rows, :], 1, 1)
            after = pltpu.roll(hz[1, rows, :], LANES - 1, 1)
            zh[rows, :] = gain * jnp.where(odd, before, after)

        def fix(i, size, beyond=None):
            done = []
            lane = lanes_of(y0)
            for q in range(size):
                p = i + q
                halo = pltpu.roll(zh[...], turn(2 * LANES - 2 * p - 1), 1)
                for t in range(nt0):
                    where = (p, t) if packed else (p,)
                    start = OWN if packed else 0
                    cols = slice(None) if packed else pl.ds(LANES * t, LANES)
                    v = dst[where + (pl.ds(start, y0), cols)]
                    if beyond is not None:
                        v = v + gain * beyond[t]
                    if t == 0:
                        v = v + jnp.where(lane == 0, halo, 0.0)
                    if t == nt0 - 1:
                        v = v + jnp.where(lane == last, halo, 0.0)
                    low, high = (gain * hy[s, t, pl.ds(p, 1), :] for s in range(2))
                    low = v[:8] + jnp.where(row8 == 0, low, 0.0)
                    high = v[y0 - 8 :] + jnp.where(row8 == 7, high, 0.0)
                    done.append((where + (pl.ds(start, 8), cols), low))
                    done.append((where + (pl.ds(start + 8, y0 - 16), cols), v[8 : y0 - 8]))
                    done.append((where + (pl.ds(start + y0 - 8, 8), cols), high))
            for where, v in done:
                dst[where] = v

        with jax.named_scope("ends"):
            fix(0, 1, hx.at[0])
            fix(x0 - 1, 1, hx.at[1])
        if not packed:
            with jax.named_scope("fix"):
                groups(1, x0 - 1, FIX_PLANES, fix)
            return []
        started = onward[0]()
        with jax.named_scope("yface"):
            for side, r0 in ((0, 0), (1, y0 - 1)):
                line = jnp.broadcast_to(zh[pl.ds(r0, 1), :], (8, LANES))
                for j in range(x0 // 8):
                    slot = 2 * (8 * j + row8)
                    low = jnp.sum(jnp.where(lane8 == slot + 1, line, 0.0), 1, keepdims=True)
                    high = jnp.sum(jnp.where(lane8 == slot, line, 0.0), 1, keepdims=True)
                    for t in range(nt0):
                        rows = (side, t, pl.ds(8 * j, 8), slice(None))
                        v = yp[rows] + gain * hy[rows]
                        if t == 0:
                            v = v + jnp.where(lane8 == 0, low, 0.0)
                        if t == nt0 - 1:
                            v = v + jnp.where(lane8 == last, high, 0.0)
                        yp[rows] = v
                for i in (0, x0 - 1):
                    for t in range(nt0):
                        yp[side, t, pl.ds(i, 1), :] = dst[i, t, pl.ds(OWN + r0, 1), :]
        started = started + onward[1]()
        with jax.named_scope("zface"):
            for k in range(nb0):
                v = zp[pl.ds(8 * k, 8), :] + zh[pl.ds(8 * k, 8), :]
                for side, kk, rr in ((0, 0, 0), (1, nb0 - 1, 7)):
                    if k == kk:
                        total = zero8
                        for j in range(x0 // 8):
                            slot = 2 * (8 * j + row8)
                            low = hy[side, 0, pl.ds(8 * j, 8), :][:, :1]
                            high = hy[side, nt0 - 1, pl.ds(8 * j, 8), :][:, last:]
                            total = total + jnp.where(lane8 == slot + 1, low, 0.0)
                            total = total + jnp.where(lane8 == slot, high, 0.0)
                        total = gain * jnp.sum(total, 0, keepdims=True)
                        v = v + jnp.where(row8 == rr, total, 0.0)
                zp[pl.ds(8 * k, 8), :] = v
            pack_z(zp, 0, dst)
            pack_z(zp, x0 - 1, dst)
        started = started + onward[2]()
        with jax.named_scope("fix"):
            groups(1, x0 - 1, FIX_PLANES, fix)
        return started

    def restrict_xy(d, low, middle, j, u_slot, first, nb, nt, dst):
        s = b["S"].at[u_slot]
        n = dst.shape[2]
        rows = pl.ds(first, 8 * nb)
        for t in range(nt):
            v = 0.25 * (d[low, t, rows, :] + d[middle + 1, t, rows, :])
            s[t, rows, :] = v + 0.5 * d[middle, t, rows, :]
        for t in range(nt):
            around = s[t, pl.ds(OWN - 1, n, stride=2), :] + s[t, pl.ds(OWN + 1, n, stride=2), :]
            dst[j, t] = 0.25 * around + 0.5 * s[t, pl.ds(OWN, n, stride=2), :]

    def restrict_planes(d, before, origin, first, nb, nt, dst):
        restrict_xy(d, before, origin, 0, 0, first, nb, nt, dst)
        for j in range(1, 4):
            restrict_xy(d, origin + 2 * j - 1, origin + 2 * j, j, j, first, nb, nt, dst)

        def some(p, _):
            for q in range(4):
                j = 4 * p + q
                restrict_xy(d, origin + 2 * j - 1, origin + 2 * j, j, q, first, nb, nt, dst)
            return 0

        lax.fori_loop(1, dst.shape[0] // 4, some, 0)

    def planes_of(src, i, chunk, rows):
        parts = [src[pl.ds(i, chunk), t, rows, :] for t in range(src.shape[1])]
        parts = [v.reshape(chunk * v.shape[1], LANES) for v in parts]
        return jnp.concatenate(parts, 1) if len(parts) > 1 else parts[0]

    def multiply(src, dst, w, first, count, chunk, rows, shift, to_rows):
        tiles = w.shape[1] // LANES

        def step(k, _):
            i = first + k * chunk
            v = dot_split(planes_of(src, i, chunk, rows), w)
            for t in range(tiles):
                part = v[:, LANES * t : LANES * t + LANES]
                dst[pl.ds(i + shift, chunk), t, to_rows, :] = part.reshape(chunk, -1, LANES)
            return 0

        if count == chunk:
            step(0, 0)
        else:
            lax.fori_loop(0, count // chunk, step, 0)

    def region(o, start, n, depth):
        lo, hi = depth
        if o == 1:
            return pl.ds(start + n - lo, lo), pl.ds(start - lo, lo)
        if o == -1:
            return pl.ds(start, hi), pl.ds(start + n, hi)
        return pl.ds(start, n), pl.ds(start, n)

    def halo_send(l, g, nx, depth_x, depth, beside):
        zpl, hzl = b[f"zp{l}"], b[f"hz{l}"]
        ny = dims[l][1]
        started = []
        for o in sorted(around, key=lambda v: -sum(map(abs, v))):
            if (o[2] != 0) == beside:
                continue
            sx, dx = region(o[0], depth_x[0], nx, depth_x)
            sy, dy = region(o[1], OWN, ny, depth)
            if beside:
                started.append(copy(g.at[sx, sy], g.at[dx, dy], o))
            else:
                side = 0 if o[2] == 1 else 1
                half = {0: (0, 2), 1: (1, 1), -1: (0, 1)}[o[0]]
                slot = {0: 0, 1: 2, -1: 3}[o[0]]
                sy = pl.ds(sy.start - OWN, sy.size)
                source = zpl.at[pl.ds(*half), sy]
                started.append(copy(source, hzl.at[side, pl.ds(slot, half[1]), dy], o))
        return started

    def merge_sides(l, left):
        hzl = b[f"hz{l}"]
        for slot in range(4):
            for k in range(ext[l][1] // 8):
                rows = pl.ds(8 * k, 8)
                v = jnp.where(left, hzl[0, slot, rows, :], hzl[1, slot, rows, :])
                hzl[0, slot, rows, :] = v

    def halo_pack1():
        g, zpl = b["G1"], b["zp1"]
        lo, hi = HALO1
        width, per = lo + hi, x1 // 2
        for half in range(2):
            total = [zero8] * (y1 // 8)
            for p in range(per):
                first = width * p
                mask = (lane8 >= first) & (lane8 < first + width)
                for k in range(y1 // 8):
                    v = pltpu.roll(g[at(lo + half * per + p, k, 0)], first + lo, 1)
                    total[k] = jnp.where(mask, v, total[k])
            for k in range(y1 // 8):
                zpl[half, pl.ds(8 * k, 8), :] = total[k]

    def halo_unpack1():
        g, hzl = b["G1"], b["hz1"]
        lo, hi = HALO1
        width, per = lo + hi, x1 // 2
        left = lane8 < lo
        for p in range(1, per):
            left = left | ((lane8 >= width * p) & (lane8 < width * p + lo))
        merge_sides(1, left)
        for e in range(-lo, x1 + hi):
            if e < 0:
                slot, p = 2, e + per
            elif e < x1:
                slot, p = e // per, e % per
            else:
                slot, p = 3, e - x1
            back = LANES - (width * p + lo)
            for k in range(ext[1][1] // 8):
                v = hzl[0, slot, pl.ds(8 * k, 8), :]
                g[at(e + lo, k, 1, 0)] = pltpu.roll(v, back % LANES, 1)

    low_pairs, high_pairs = -(-HALO2[0] // 2), -(-HALO2[1] // 2)
    pairs, per2 = x2 // 2, x2 // 4
    assert sum(HALO2) <= 16 and per2 <= 4 and max(low_pairs, high_pairs) <= per2

    def halo_pack2():
        p2, zpl = b["P2"], b["zp2"]
        lo, hi = HALO2
        for half in range(2):
            total = [zero8] * (y2 // 8)
            for p in range(per2):
                first = lane8 % (LANES // 2) - 16 * p
                mask = (first >= 0) & (first < lo + hi)
                for k in range(y2 // 8):
                    v = p2[low_pairs + half * per2 + p, pl.ds(OWN + 8 * k, 8), :]
                    v = pltpu.roll(v, 16 * p + lo, 1)
                    total[k] = jnp.where(mask, v, total[k])
            for k in range(y2 // 8):
                zpl[half, pl.ds(8 * k, 8), :] = total[k]

    def halo_unpack2():
        g, p2, hzl = b["G2"], b["P2"], b["hz2"]
        lo, hi = HALO2
        half_lanes = LANES // 2
        for e in range(-lo, x2 + hi):
            pair, odd = (e + 2 * low_pairs) // 2, e % 2
            q = pair - low_pairs
            if q < 0:
                slot, p = 2, q + per2
            elif q < pairs:
                slot, p = q // per2, q % per2
            else:
                slot, p = 3, q - pairs
            back = LANES - (16 * p + lo) + (0 if odd else half_lanes)
            for k in range(ext[2][1] // 8):
                rows = pl.ds(8 * k, 8)
                own = p2[pair, rows, :]
                own = pltpu.roll(own, half_lanes, 1) if odd else own
                low = pltpu.roll(hzl[0, slot, rows, :], back % LANES, 1)
                high = pltpu.roll(hzl[1, slot, rows, :], back % LANES, 1)
                v = jnp.where(lane8 < 3 * half_lanes // 2, high, low)
                g[at(e + lo, k, 0, 0)] = jnp.where(lane8 < half_lanes, own, v)

    def ext_sweep(mode, l, src, dst, size, reach):
        nt, origin = ext[l][2], ext[l][3]
        nx, ny, _ = dims[l]
        g = b[f"G{l}"]
        first = OWN - reach[0]
        rows = 8 * -(-(ny + sum(reach)) // 8)

        def some(i, count):
            for q in range(count):
                p = i + q
                new = stencil(mode, l, src, g, p, (p - 1, p + 1), first, rows, nt, True)
                for t, value in enumerate(new):
                    dst[p, t, pl.ds(first, rows), :] = value

        groups(origin - reach[0], origin + nx + reach[1], size, some)

    def spread_rows(q, v, j, c0, t):
        c, n = q[at(j, 0, t, OWN + c0)], q[at(j, 0, t, OWN + c0 + 1)]
        return c, 0.5 * (c + n)

    st, sg = b["stats"], [b[f"sums{a}"] for a in range(3)]

    def spread_sums(a):
        return [
            copy(st.at[a], sg[a].at[j], tuple(j if i == a else 0 for i in range(3)))
            for j in range(1, counts[a])
        ]

    def gather_sums(a, copies):
        wait(copies)
        total = st[a]
        for j in range(1, counts[a]):
            total = total + sg[a][j]
        if a < 2:
            st[a + 1] = total
        return total

    def fold(ref):
        def step(p, totals):
            totals = list(totals)
            for q in range(2):
                for k in range(nb0):
                    for t in range(nt0):
                        totals[(2 * k + t) % 4] += ref[at(2 * p + q, k, t)]
            return tuple(totals)

        t = lax.fori_loop(0, x0 // 2, step, (zero8,) * 4)
        return (t[0] + t[1]) + (t[2] + t[3])

    a1, b1, g1 = b["A1"], b["B1"], b["G1"]
    a2, b2, g2 = b["A2"], b["B2"], b["G2"]

    with jax.named_scope("clear"):

        def clear0(i, _):
            for ref in (u, a0, b0):
                for t in range(nt0):
                    ref[i, t, pl.ds(0, OWN), :] = zero8
                    ref[i, t, pl.ds(OWN + y0, OWN), :] = zero8
            return 0

        lax.fori_loop(0, x0, clear0, 0)
        for l in (1, 2):
            ex, ey, tiles, _ = ext[l]
            refs = [b[f"{name}{l}"] for name in "GAB"]

            def clear(i, _, refs=refs, ey=ey, tiles=tiles):
                for ref in refs:
                    for k in range(ey // 8):
                        for t in range(tiles):
                            ref[at(i, k, t, 0)] = zero8
                return 0

            lax.fori_loop(0, ex, clear, 0)
            for side in range(2):
                for slot in range(4):
                    for k in range(ey // 8):
                        b[f"hz{l}"][side, slot, pl.ds(8 * k, 8), :] = zero8
        for p in range(b["P2"].shape[0]):
            for k in range(ext[2][1] // 8):
                b["P2"][p, pl.ds(8 * k, 8), :] = zero8
    with jax.named_scope("loadu"):
        loads[0].wait()
        loads[1].wait()
    with jax.named_scope("packu"):

        def pack_some(i, count):
            for q in range(count):
                pack_z(b["zp"].at[0], i + q, u)

        groups(0, x0, 8, pack_some)
    with jax.named_scope("sumu"):
        st[0, 0] = fold(u)
    with jax.named_scope("barrier"):
        pl.semaphore_wait(barrier, len(offsets))
    send_x, send_y, send_z = exchange(0, u)
    moving = send_x() + send_y() + send_z()
    with jax.named_scope("sumf"):
        loads[2].wait()
        loads[3].wait()
        st[0, 1] = fold(f)
    sums = spread_sums(0)
    faces = b["yp"]
    moving = sweep(0, moving, u, a0, exchange(1, a0, faces.at[1]))
    gather_sums(0, sums)
    sums = spread_sums(1)
    moving = sweep(1, moving, a0, b0, exchange(2, b0, faces.at[0]))
    gather_sums(1, sums)
    sums = spread_sums(2)
    moving = sweep(2, moving, b0, d0, defect_exchange(3, d0), mode="defect")
    total = gather_sums(2, sums)
    mean_u = jnp.sum(total[0]) * (1.0 / cells)
    mean_f = jnp.sum(total[1]) * (1.0 / cells)
    wait(moving)

    with jax.named_scope("restrict0"):
        lane = lax.broadcasted_iota(jnp.int32, (y0 + 8, LANES), 1)
        moved = pltpu.roll(b["rw"][...], 1, 1)
        rim = jnp.where(lane == last, moved, b["rz"][...])
        b["m"][...] = dot_split(rim, restrict_matrix(LANES, LANES, x1, last, 2))
        m = b["m"]
        v = 0.25 * (m[pl.ds(OWN - 1, y1, stride=2), :] + m[pl.ds(OWN + 1, y1, stride=2), :])
        b["n"][...] = 0.25 * (v + 0.5 * m[pl.ds(OWN, y1, stride=2), :])
        restrict_planes(d0, x0, 0, 0, nb0 + 1, nt0, b["T0"])
        w = restrict_matrix(z0, LANES, z1)
        o1, own1 = ext[1][3], pl.ds(OWN, y1)
        multiply(b["T0"], g1, w, 0, x1, 8, pl.ds(0, y1), o1, own1)

        def finish(i, count):
            for q in range(count):
                for k in range(y1 // 8):
                    col = pltpu.roll(b["n"][pl.ds(8 * k, 8), :], turn(2 * LANES - (i + q)), 1)
                    where = at(i + q + o1, k, 0)
                    g1[where] = g1[where] + jnp.where(lane8 == 0, col, 0.0) - mean_f

        groups(0, x1, 8, finish)
    moving = halo_send(1, g1.at[:, 0], x1, HALO1, HALO1, True)
    with jax.named_scope("pack1"):
        halo_pack1()
    moving = moving + halo_send(1, g1.at[:, 0], x1, HALO1, HALO1, False)
    wait(moving)
    with jax.named_scope("unpack1"):
        halo_unpack1()
    with jax.named_scope("first1"):
        ext_sweep("first", 1, g1, b1, 19, (2, 3))
    with jax.named_scope("defect1"):
        ext_sweep("defect", 1, b1, a1, 19, (1, 0))
    with jax.named_scope("restrict1"):
        t1 = b["T1"]
        blocks1 = -(-(y1 + 1) // 8)
        restrict_planes(a1, o1 - 1, o1, OWN - 1, blocks1, 2, t1)
        w = restrict_matrix(2 * LANES, LANES // 2, z2, 2 * LANES - 1)
        none = jnp.zeros_like(w)
        w = jnp.concatenate([jnp.concatenate([w, none], 1), jnp.concatenate([none, w], 1)], 0)
        paired = []
        for half in range(2):
            for t in range(2):
                v = [t1[2 * p + half, t] for p in range(pairs)]
                paired.append(jnp.concatenate(v, 0))
        v = dot_split(jnp.concatenate(paired, 1), w).reshape(pairs, y2, LANES)
        b["P2"][pl.ds(low_pairs, pairs), pl.ds(OWN, y2), :] = v
    depth2 = (low_pairs, high_pairs)
    moving = halo_send(2, b["P2"], pairs, depth2, HALO2, True)
    with jax.named_scope("pack2"):
        halo_pack2()
    moving = moving + halo_send(2, b["P2"], pairs, depth2, HALO2, False)
    wait(moving)
    with jax.named_scope("unpack2"):
        halo_unpack2()
    with jax.named_scope("sweeps2"):
        v, w2 = a2, b2
        reach = [(k + 1, k + 2) for k in range(COARSE_SWEEPS - 1)][::-1]
        ext_sweep("first", 2, g2, v, 27, reach[0])
        for k in range(1, COARSE_SWEEPS - 1):
            ext_sweep("relax", 2, v, w2, 27, reach[k])
            v, w2 = w2, v
    with jax.named_scope("prolong1"):
        o2 = ext[2][3]
        q1, v1 = b["Q1"], b["V1"]
        w = prolong_matrix(LANES, 2 * LANES, z1, True)
        multiply(v, q1, w, o2 - 1, x2 + 3, x2 + 3, pl.ds(0, ext[2][1]), 0, pl.ds(0, ext[2][1]))

        def spread1(i, count):
            for q in range(count):
                for t in range(2):
                    for c0 in range(-2, (y1 + 3) // 2, 8):
                        even, odd = spread_rows(q1, v1, i + q, c0, t)
                        v1[i + q, t, pl.ds(OWN + 2 * c0, 8, stride=2), :] = even
                        v1[i + q, t, pl.ds(OWN + 2 * c0 + 1, 8, stride=2), :] = odd

        groups(o2 - 1, o2 + x2 + 2, 5, spread1)

        def add1(i, count):
            for q in range(count):
                j = i + q
                for k in range(-(-(y1 + 5) // 8)):
                    for t in range(2):
                        c = v1[at(j + o2, k, t, OWN - 2)]
                        n = v1[at(j + 1 + o2, k, t, OWN - 2)]
                        even, odd = (at(2 * j + o1 + p, k, t, OWN - 2) for p in range(2))
                        b1[even] = b1[even] + c
                        b1[odd] = b1[odd] + 0.5 * (c + n)

        add1(-1, 1)
        groups(0, x2 + 1, 2, add1)
        for k in range(-(-(y1 + 5) // 8)):
            for t in range(2):
                even = at(x1 + 2 + o1, k, t, OWN - 2)
                b1[even] = b1[even] + v1[at(x2 + 1 + o2, k, t, OWN - 2)]
    with jax.named_scope("post1"):
        ext_sweep("relax", 1, b1, a1, 19, (1, 2))
        ext_sweep("relax", 1, a1, b1, 19, (0, 1))
    with jax.named_scope("prolong0"):
        q0, v0 = b["Q0"], b["V0"]
        w = prolong_matrix(2 * LANES, z0, z0, False)
        rows = pl.ds(OWN, y1 + 8)
        multiply(b1, q0, w, o1, x1 + 1, 3, rows, -o1, rows)

        def spread0(i, count):
            for q in range(count):
                for t in range(nt0):
                    for c0 in range(0, y1, 8):
                        even, odd = spread_rows(q0, v0, i + q, c0, t)
                        v0[i + q, t, pl.ds(2 * c0, 8, stride=2), :] = even
                        v0[i + q, t, pl.ds(2 * c0 + 1, 8, stride=2), :] = odd

        groups(0, x1 + 1, 3, spread0)
        shift = mean_u + 2.0 * W * mean_f

        def add0(i, count):
            for q in range(count):
                j = i + q
                for k in range(nb0):
                    for t in range(nt0):
                        c = v0[at(j, k, t, 0)] - shift
                        n = v0[at(j + 1, k, t, 0)] - shift
                        even, odd = at(2 * j, k, t), at(2 * j + 1, k, t)
                        b0[even] = b0[even] + c
                        b0[odd] = b0[odd] + 0.5 * (c + n)

        send_x, send_y, send_z = exchange(3, b0)
        add0(0, 1)
        add0(x1 - 1, 1)
        moving = send_x()
        groups(1, x1 - 1, 2, add0)
        moving = moving + send_y()

        def pack_b0(i, count):
            for q in range(count):
                pack_z(b["zp"].at[1], i + q, b0)

        groups(0, x0, 8, pack_b0)
        moving = moving + send_z()
    moving = sweep(3, moving, b0, a0, exchange(4, a0, faces.at[0]), shift=W * mean_f)
    sweep(4, moving, a0, out, shift=W * mean_f)


def solution(mesh):
    counts = tuple(mesh.shape[a] for a in AXES)

    def shards(right_side, initial_guess):
        shape = right_side.shape
        dims = tuple(tuple(n >> l for n in shape) for l in range(3))
        cells = float(right_side.size)
        for n in counts:
            cells *= n
        bufs = buffers(dims, counts)
        messages = 5 * 6 + 4 + 9 + 2 * 26 + sum(counts) - 3
        return pl.pallas_call(
            functools.partial(kernel, dims, counts, tuple(bufs), cells),
            out_shape=jax.ShapeDtypeStruct(shape, jnp.float32),
            in_specs=[pl.BlockSpec(memory_space=pl.ANY)] * 2,
            out_specs=pl.BlockSpec(memory_space=pltpu.VMEM),
            scratch_shapes=list(bufs.values())
            + [pltpu.SemaphoreType.DMA((n,)) for n in (messages, messages, 4)],
            compiler_params=pltpu.CompilerParams(
                collective_id=0, has_side_effects=True, vmem_limit_bytes=56 * 1024 * 1024
            ),
        )(initial_guess, right_side)

    placed = (P(*AXES), P(*AXES))
    return jax.shard_map(
        shards, mesh=mesh, in_specs=placed, out_specs=P(*AXES), check_vma=False
    )
```

```python
import functools
import itertools

import jax
import jax.numpy as jnp
from jax import lax
from jax.experimental import pallas as pl
from jax.experimental.pallas import tpu as pltpu
from jax.sharding import PartitionSpec as P

COARSE_SWEEPS = 6
LANES = 128
AXES = ("gx", "gy", "gz")
relax_weight = 0.8
W = relax_weight / 6.0

SWEEP_PLANES = 10
FIX_PLANES = 12

HALO1 = (4, 5)
HALO2 = (COARSE_SWEEPS + 1, COARSE_SWEEPS + 2)


def dot_split(a, w):
    hi = a.astype(jnp.bfloat16)
    mid = (a - hi.astype(jnp.float32)).astype(jnp.bfloat16)
    dot = functools.partial(jnp.dot, preferred_element_type=jnp.float32)
    return dot(hi, w) + dot(mid, w)


def iotas(shape):
    return (
        lax.broadcasted_iota(jnp.int32, shape, 0),
        lax.broadcasted_iota(jnp.int32, shape, 1),
    )


def restrict_matrix(rows, cols, count, wrap=None, step=1):
    r, c = iotas((rows, cols))
    d = jnp.abs(r - 2 * step * c)
    w = jnp.where(d == 0, 0.5, 0.0) + jnp.where(d == step, 0.25, 0.0)
    w = jnp.where((c < count) & (r < 2 * step * count), w, 0.0)
    if wrap is not None:
        w = w + jnp.where((r == wrap) & (c == 0), 0.25, 0.0)
    return w.astype(jnp.bfloat16)


def prolong_matrix(rows, cols, fine, wrapped):
    r, c = iotas((rows, cols))
    if wrapped:
        r = jnp.where(r < 3 * rows // 4, r, r - rows)
        c = jnp.where(c < 3 * cols // 4, c, c - cols)
    d = jnp.abs(c - 2 * r)
    w = jnp.where(d == 0, 1.0, 0.0) + jnp.where(d == 1, 0.5, 0.0)
    return w.astype(jnp.bfloat16)


def hat_matrices(rows, cols):
    r, c = iotas((rows, cols))
    d = jnp.abs(c - 2 * jnp.where(r < 3 * rows // 4, r, r - rows))
    parts = []
    for row in ((1.0, 0.5), (1.0, 1.0, 0.5), (2.0, 1.5, 1.0, 0.5)):
        w = jnp.zeros((rows, cols), jnp.float32)
        for k, value in enumerate(row):
            w = w + jnp.where(d == k, value, 0.0)
        parts.append(w.astype(jnp.bfloat16))
    return jnp.concatenate(parts, 1)


def turn(by):
    return by % LANES if isinstance(by, int) else lax.rem(by, LANES)


OWN = 8


def extended(dims):
    (x1, y1, _), (x2, y2, _) = dims[1], dims[2]
    up = lambda n: -(-n // 8) * 8
    return (
        None,
        (x1 + sum(HALO1), up(y1 + OWN + HALO1[1] + 9), 2, HALO1[0]),
        (x2 + sum(HALO2), up(y2 + OWN + HALO2[1] + 4), 1, HALO2[0]),
    )


def buffers(dims, counts):
    (x, y, z), (x1, y1, _), (x2, y2, _) = dims
    ext = extended(dims)
    nt = z // LANES
    out = {}
    for name in ("u", "f", "A0", "B0"):
        out[name] = (x, nt, y + 2 * OWN, LANES)
    out["D0"] = (x + 1, nt, y + OWN, LANES)
    out["yp"] = (2, 2, nt, x, LANES)
    out["zp"] = (2, y, LANES)
    out["zh"] = (y, LANES)
    out["hx"] = (5, 2, nt, y, LANES)
    out["hy"] = (5, 2, nt, x, LANES)
    out["hz"] = (5, 2, y, LANES)
    out["rz"] = (y + OWN, LANES)
    out["rw"] = (y + OWN, LANES)
    out["m"] = (y + OWN, LANES)
    out["n"] = (y // 2, LANES)
    out["S"] = (4, nt, y + OWN, LANES)
    out["T0"] = (x1, nt, y1, LANES)
    out["T1"] = (x2, 2, y2, LANES)
    for l, ny in ((1, y1), (2, y2)):
        ex, ey, tiles, _ = ext[l]
        for name in "GAB":
            out[f"{name}{l}"] = (ex, tiles, ey, LANES)
        packs = 2 if l == 2 else -(-x1 * sum(HALO1) // LANES)
        out[f"zp{l}"] = (packs, ny, LANES)
        out[f"hz{l}"] = (2, packs + 2, ey, LANES)
    out["P2"] = (x2 // 2 + -(-HALO2[0] // 2) + -(-HALO2[1] // 2), ext[2][1], LANES)
    out["Q1"] = (ext[2][0], 2, ext[2][1], LANES)
    out["V1"] = (ext[2][0], 2, ext[1][1] + 8, LANES)
    for name in ("CA", "CB", "CC"):
        out[name] = (x1 + 3, nt, ext[1][1], LANES)
    out["stats"] = (3, 2, 8, LANES)
    for a in range(3):
        out[f"sums{a}"] = (counts[a], 2, 8, LANES)
    return {k: pltpu.VMEM(v, jnp.float32) for k, v in out.items()}


def kernel(dims, counts, names, cells, u_far, f_far, out, *scratch):
    b = dict(zip(names, scratch[:-3]))
    send_sem, recv_sem, load_sem = scratch[-3:]
    u, f, a0, b0, d0 = b["u"], b["f"], b["A0"], b["B0"], b["D0"]
    loads = []
    for n, (far, near) in enumerate(((u_far, u), (f_far, f))):
        for t in range(2):
            lanes = pl.ds(LANES * t, LANES)
            own = near.at[:, t, pl.ds(OWN, dims[0][1]), :]
            c = pltpu.make_async_copy(far.at[:, :, lanes], own, load_sem.at[2 * n + t])
            c.start()
            loads.append(c)
    here = {a: lax.axis_index(a) for a in AXES}
    serial = itertools.count()
    ext = extended(dims)
    x0, y0, z0 = dims[0]
    x1, y1, z1 = dims[1]
    x2, y2, z2 = dims[2]
    nb0, nt0 = y0 // 8, z0 // LANES
    assert 2 * x0 == LANES and z1 == LANES and 2 * z2 == LANES
    assert nt0 == 2 and y2 % 8 == 0

    def device(offset):
        return tuple(lax.rem(here[a] + (o % n), n) for a, o, n in zip(AXES, offset, counts))

    def copy(src, dst, offset):
        k = next(serial)
        c = pltpu.make_async_remote_copy(
            src_ref=src,
            dst_ref=dst,
            send_sem=send_sem.at[k],
            recv_sem=recv_sem.at[k],
            device_id=device(offset),
            device_id_type=pl.DeviceIdType.MESH,
        )
        c.start()
        return c

    def wait(copies):
        with jax.named_scope("wait"):
            for c in copies:
                c.wait()

    around = [o for o in itertools.product((-1, 0, 1), repeat=3) if any(o)]
    offsets = list(around)
    for a in range(3):
        for j in range(2, counts[a] - 1):
            offsets.append(tuple(j if i == a else 0 for i in range(3)))
    barrier = pltpu.get_barrier_semaphore()
    for o in offsets:
        pl.semaphore_signal(
            barrier, inc=1, device_id=device(o), device_id_type=pl.DeviceIdType.MESH
        )

    row8 = lax.broadcasted_iota(jnp.int32, (8, LANES), 0)
    lane8 = lax.broadcasted_iota(jnp.int32, (8, LANES), 1)
    zero8 = jnp.zeros((8, LANES), jnp.float32)

    def at(i, k, t, first=OWN):
        return i, t, pl.ds(first + 8 * k, 8), slice(None)

    def groups(lo, hi, size, body):
        steps = (hi - lo) // size

        def step(p, _):
            body(lo + size * p, size)
            return 0

        if steps > 1:
            lax.fori_loop(0, steps, step, 0)
        elif steps:
            body(lo, size)
        if (hi - lo) % size:
            body(lo + size * steps, (hi - lo) % size)

    def lanes_of(rows):
        return lax.broadcasted_iota(jnp.int32, (rows, LANES), 1)

    def stencil(mode, l, src, g, i, near, first, rows, nt, z_wrap, shift=None):
        scale = 0.25**l
        lane = lanes_of(rows)
        here, above, below = (pl.ds(first + d, rows) for d in (0, -1, 1))
        c = [src[i, t, here, :] for t in range(nt)]
        left = [pltpu.roll(v, 1, 1) for v in c]
        right = [pltpu.roll(v, LANES - 1, 1) for v in c]
        new = []
        for t in range(nt):
            v = c[t]
            s = src[i, t, above, :] + src[i, t, below, :]
            for j in near:
                s = s + src[j, t, here, :]
            if z_wrap and nt == 1:
                s = s + (left[t] + right[t])
            else:
                before = left[t - 1] if t or z_wrap else 0.0
                after = right[(t + 1) % nt] if t < nt - 1 or z_wrap else 0.0
                z = jnp.where(lane == 0, before, left[t])
                s = s + (z + jnp.where(lane == LANES - 1, after, right[t]))
            if mode == "first":
                z = W / scale
                value = (W * z) * s + (W * (1.5 * z + 1.0 / scale)) * v
            elif mode == "defect":
                value = s - 6.0 * v
                value = g[i, t, here, :] + (value if l == 0 else scale * value)
            else:
                gv = g[i, t, here, :]
                value = s + 1.5 * v
                value = W * (value + (gv if l == 0 else (1.0 / scale) * gv))
                if shift is not None:
                    value = value - shift
            new.append(value)
        return new

    zh = b["zh"]
    last = LANES - 1

    def pack_z(zp, i, ref):
        lane = lanes_of(y0)
        both = jnp.where(lane == last, ref[i, nt0 - 1, own0, :], ref[i, 0, own0, :])
        moved = pltpu.roll(both, turn(2 * i + 1), 1)
        pltpu.store(zp, moved, mask=(lane == 2 * i) | (lane == 2 * i + 1))

    def pack_rows(yp, i, new):
        for side, r in ((0, 0), (1, y0 - 1)):
            for t in range(nt0):
                yp[side, t, pl.ds(i, 1), :] = new[t][r : r + 1]

    own0 = pl.ds(OWN, y0)

    def exchange(r, src, faces=None):
        hx, hy, hz = b["hx"].at[r], b["hy"].at[r], b["hz"].at[r]
        zp = b["zp"].at[r % 2]

        def send_x():
            return [
                copy(src.at[x0 - 1, :, own0], hx.at[0], (1, 0, 0)),
                copy(src.at[0, :, own0], hx.at[1], (-1, 0, 0)),
            ]

        def send_y():
            if faces is not None:
                return [
                    copy(faces.at[1], hy.at[0], (0, 1, 0)),
                    copy(faces.at[0], hy.at[1], (0, -1, 0)),
                ]
            started = []
            for t in range(nt0):
                started.append(copy(src.at[:, t, OWN + y0 - 1], hy.at[0, t], (0, 1, 0)))
                started.append(copy(src.at[:, t, OWN], hy.at[1, t], (0, -1, 0)))
            return started

        def send_z():
            return [
                copy(zp, hz.at[0], (0, 0, 1)),
                copy(zp, hz.at[1], (0, 0, -1)),
            ]

        return send_x, send_y, send_z

    def defect_exchange(r, d):
        rz, rw = b["rz"], b["rw"]
        yp, zp = b["yp"].at[r % 2], b["zp"].at[r % 2]

        def send_x():
            return [copy(d.at[x0 - 1, :, own0], d.at[x0, :, own0], (1, 0, 0))]

        def send_y():
            started = []
            for t in range(nt0):
                started.append(copy(yp.at[1, t, x0 - 1], d.at[x0, t, OWN - 1], (1, 1, 0)))
                started.append(copy(yp.at[1, t], d.at[pl.ds(0, x0), t, OWN - 1], (0, 1, 0)))
            return started

        def send_z():
            end, before = zp.at[pl.ds(y0 - 1, 1)], pl.ds(OWN - 1, 1)
            return [
                copy(end, rw.at[before], (1, 1, 1)),
                copy(zp, rw.at[own0], (1, 0, 1)),
                copy(end, rz.at[before], (0, 1, 1)),
                copy(zp, rz.at[own0], (0, 0, 1)),
            ]

        return send_x, send_y, send_z

    def sweep(r, moving, src, dst, onward=None, mode="relax", shift=None):
        hx, hy, hz = b["hx"].at[r], b["hy"].at[r], b["hz"].at[r]
        yp, zp = b["yp"].at[(r + 1) % 2], b["zp"].at[(r + 1) % 2]
        gain = 1.0 if mode == "defect" else W
        packed = onward is not None

        def plane(i, near):
            new = stencil(mode, 0, src, f, i, near, OWN, y0, nt0, False, shift)
            for t, value in enumerate(new):
                dst[i, t, own0, :] = value
            if packed:
                pack_rows(yp, i, new)

        def some(i, count):
            for q in range(count):
                plane(i + q, (i + q - 1, i + q + 1))
            if packed:
                for q in range(count):
                    pack_z(zp, i + q - 2, dst)

        with jax.named_scope("inner"):
            plane(0, (1,))
            plane(x0 - 1, (x0 - 2,))
            plane(1, (0, 2))
            plane(2, (1, 3))
            groups(3, x0 - 1, SWEEP_PLANES, some)
            if packed:
                pack_z(zp, x0 - 3, dst)
                pack_z(zp, x0 - 2, dst)
        wait(moving)
        odd = lane8 % 2 == 1
        for k in range(nb0):
            rows = pl.ds(8 * k, 8)
            before = pltpu.roll(hz[0, rows, :], 1, 1)
            after = pltpu.roll(hz[1, rows, :], LANES - 1, 1)
            zh[rows, :] = gain * jnp.where(odd, before, after)

        def fix(i, size, beyond=None):
            done = []
            lane = lanes_of(y0)
            for q in range(size):
                p = i + q
                halo = pltpu.roll(zh[...], turn(2 * LANES - 2 * p - 1), 1)
                for t in range(nt0):
                    v = dst[p, t, own0, :]
                    if beyond is not None:
                        v = v + gain * beyond[t]
                    if t == 0:
                        v = v + jnp.where(lane == 0, halo, 0.0)
                    if t == nt0 - 1:
                        v = v + jnp.where(lane == last, halo, 0.0)
                    low, high = (gain * hy[s, t, pl.ds(p, 1), :] for s in range(2))
                    low = v[:8] + jnp.where(row8 == 0, low, 0.0)
                    high = v[y0 - 8 :] + jnp.where(row8 == 7, high, 0.0)
                    done.append((p, t, OWN, low))
                    done.append((p, t, OWN + 8, v[8 : y0 - 8]))
                    done.append((p, t, OWN + y0 - 8, high))
            for p, t, start, v in done:
                dst[p, t, pl.ds(start, v.shape[0]), :] = v

        with jax.named_scope("ends"):
            fix(0, 1, hx.at[0])
            fix(x0 - 1, 1, hx.at[1])
        if not packed:
            with jax.named_scope("fix"):
                groups(1, x0 - 1, FIX_PLANES, fix)
            return []
        started = onward[0]()
        with jax.named_scope("yface"):
            for side, r0 in ((0, 0), (1, y0 - 1)):
                line = jnp.broadcast_to(zh[pl.ds(r0, 1), :], (8, LANES))
                for j in range(x0 // 8):
                    slot = 2 * (8 * j + row8)
                    low = jnp.sum(jnp.where(lane8 == slot + 1, line, 0.0), 1, keepdims=True)
                    high = jnp.sum(jnp.where(lane8 == slot, line, 0.0), 1, keepdims=True)
                    for t in range(nt0):
                        rows = (side, t, pl.ds(8 * j, 8), slice(None))
                        v = yp[rows] + gain * hy[rows]
                        if t == 0:
                            v = v + jnp.where(lane8 == 0, low, 0.0)
                        if t == nt0 - 1:
                            v = v + jnp.where(lane8 == last, high, 0.0)
                        yp[rows] = v
                for i in (0, x0 - 1):
                    for t in range(nt0):
                        yp[side, t, pl.ds(i, 1), :] = dst[i, t, pl.ds(OWN + r0, 1), :]
        started = started + onward[1]()
        with jax.named_scope("zface"):
            for k in range(nb0):
                v = zp[pl.ds(8 * k, 8), :] + zh[pl.ds(8 * k, 8), :]
                for side, kk, rr in ((0, 0, 0), (1, nb0 - 1, 7)):
                    if k == kk:
                        total = zero8
                        for j in range(x0 // 8):
                            slot = 2 * (8 * j + row8)
                            low = hy[side, 0, pl.ds(8 * j, 8), :][:, :1]
                            high = hy[side, nt0 - 1, pl.ds(8 * j, 8), :][:, last:]
                            total = total + jnp.where(lane8 == slot + 1, low, 0.0)
                            total = total + jnp.where(lane8 == slot, high, 0.0)
                        total = gain * jnp.sum(total, 0, keepdims=True)
                        v = v + jnp.where(row8 == rr, total, 0.0)
                zp[pl.ds(8 * k, 8), :] = v
            pack_z(zp, 0, dst)
            pack_z(zp, x0 - 1, dst)
        started = started + onward[2]()
        with jax.named_scope("fix"):
            groups(1, x0 - 1, FIX_PLANES, fix)
        return started

    def restrict_xy(d, low, middle, j, u_slot, first, nb, nt, dst):
        s = b["S"].at[u_slot]
        n = dst.shape[2]
        rows = pl.ds(first, 8 * nb)
        for t in range(nt):
            v = 0.25 * (d[low, t, rows, :] + d[middle + 1, t, rows, :])
            s[t, rows, :] = v + 0.5 * d[middle, t, rows, :]
        for t in range(nt):
            around = s[t, pl.ds(OWN - 1, n, stride=2), :] + s[t, pl.ds(OWN + 1, n, stride=2), :]
            dst[j, t] = 0.25 * around + 0.5 * s[t, pl.ds(OWN, n, stride=2), :]

    def restrict_planes(d, before, origin, first, nb, nt, dst):
        restrict_xy(d, before, origin, 0, 0, first, nb, nt, dst)
        for j in range(1, 4):
            restrict_xy(d, origin + 2 * j - 1, origin + 2 * j, j, j, first, nb, nt, dst)

        def some(p, _):
            for q in range(4):
                j = 4 * p + q
                restrict_xy(d, origin + 2 * j - 1, origin + 2 * j, j, q, first, nb, nt, dst)
            return 0

        lax.fori_loop(1, dst.shape[0] // 4, some, 0)

    def planes_of(src, i, chunk, rows):
        parts = [src[pl.ds(i, chunk), t, rows, :] for t in range(src.shape[1])]
        parts = [v.reshape(chunk * v.shape[1], LANES) for v in parts]
        return jnp.concatenate(parts, 1) if len(parts) > 1 else parts[0]

    def multiply(src, dst, w, first, count, chunk, rows, shift, to_rows):
        tiles = w.shape[1] // LANES

        def step(k, _):
            i = first + k * chunk
            v = dot_split(planes_of(src, i, chunk, rows), w)
            for t in range(tiles):
                part = v[:, LANES * t : LANES * t + LANES]
                dst[pl.ds(i + shift, chunk), t, to_rows, :] = part.reshape(chunk, -1, LANES)
            return 0

        if count == chunk:
            step(0, 0)
        else:
            lax.fori_loop(0, count // chunk, step, 0)

    def region(o, start, n, depth):
        lo, hi = depth
        if o == 1:
            return pl.ds(start + n - lo, lo), pl.ds(start - lo, lo)
        if o == -1:
            return pl.ds(start, hi), pl.ds(start + n, hi)
        return pl.ds(start, n), pl.ds(start, n)

    def halo_send(l, g, nx, depth_x, depth, beside):
        zpl, hzl = b[f"zp{l}"], b[f"hz{l}"]
        ny = dims[l][1]
        started = []
        for o in sorted(around, key=lambda v: -sum(map(abs, v))):
            if (o[2] != 0) == beside:
                continue
            sx, dx = region(o[0], depth_x[0], nx, depth_x)
            sy, dy = region(o[1], OWN, ny, depth)
            if beside:
                started.append(copy(g.at[sx, sy], g.at[dx, dy], o))
            else:
                side = 0 if o[2] == 1 else 1
                packs = zpl.shape[0]
                half = {0: (0, packs), 1: (packs - 1, 1), -1: (0, 1)}[o[0]]
                slot = {0: 0, 1: packs, -1: packs + 1}[o[0]]
                sy = pl.ds(sy.start - OWN, sy.size)
                source = zpl.at[pl.ds(*half), sy]
                started.append(copy(source, hzl.at[side, pl.ds(slot, half[1]), dy], o))
        return started

    def merge_sides(l, left):
        hzl = b[f"hz{l}"]
        for slot in range(hzl.shape[1]):
            for k in range(ext[l][1] // 8):
                rows = pl.ds(8 * k, 8)
                v = jnp.where(left, hzl[0, slot, rows, :], hzl[1, slot, rows, :])
                hzl[0, slot, rows, :] = v

    def halo_pack1():
        g, zpl = b["G1"], b["zp1"]
        lo, hi = HALO1
        width, packs = lo + hi, zpl.shape[0]
        per = -(-x1 // packs)
        for half in range(packs):
            total = [zero8] * (y1 // 8)
            for p in range(min(per, x1 - half * per)):
                first = width * p
                mask = (lane8 >= first) & (lane8 < first + width)
                for k in range(y1 // 8):
                    v = pltpu.roll(g[at(lo + half * per + p, k, 0)], first + lo, 1)
                    total[k] = jnp.where(mask, v, total[k])
            for k in range(y1 // 8):
                zpl[half, pl.ds(8 * k, 8), :] = total[k]

    def halo_unpack1():
        g, hzl = b["G1"], b["hz1"]
        lo, hi = HALO1
        width, packs = lo + hi, hzl.shape[1] - 2
        per = -(-x1 // packs)
        assert per * width <= LANES and hi <= per and lo <= x1 - (packs - 1) * per
        left = lane8 < lo
        for p in range(1, per):
            left = left | ((lane8 >= width * p) & (lane8 < width * p + lo))
        merge_sides(1, left)
        for e in range(-lo, x1 + hi):
            if e < 0:
                slot, p = packs, x1 + e - (packs - 1) * per
            elif e < x1:
                slot, p = e // per, e % per
            else:
                slot, p = packs + 1, e - x1
            back = LANES - (width * p + lo)
            for k in range(ext[1][1] // 8):
                v = hzl[0, slot, pl.ds(8 * k, 8), :]
                g[at(e + lo, k, 1, 0)] = pltpu.roll(v, back % LANES, 1)

    low_pairs, high_pairs = -(-HALO2[0] // 2), -(-HALO2[1] // 2)
    pairs, per2 = x2 // 2, x2 // 4
    assert sum(HALO2) <= 16 and per2 <= 4 and max(low_pairs, high_pairs) <= per2

    def halo_pack2():
        p2, zpl = b["P2"], b["zp2"]
        lo, hi = HALO2
        for half in range(2):
            total = [zero8] * (y2 // 8)
            for p in range(per2):
                first = lane8 % (LANES // 2) - 16 * p
                mask = (first >= 0) & (first < lo + hi)
                for k in range(y2 // 8):
                    v = p2[low_pairs + half * per2 + p, pl.ds(OWN + 8 * k, 8), :]
                    v = pltpu.roll(v, 16 * p + lo, 1)
                    total[k] = jnp.where(mask, v, total[k])
            for k in range(y2 // 8):
                zpl[half, pl.ds(8 * k, 8), :] = total[k]

    def halo_unpack2():
        g, p2, hzl = b["G2"], b["P2"], b["hz2"]
        lo, hi = HALO2
        half_lanes = LANES // 2
        for e in range(-lo, x2 + hi):
            pair, odd = (e + 2 * low_pairs) // 2, e % 2
            q = pair - low_pairs
            if q < 0:
                slot, p = 2, q + per2
            elif q < pairs:
                slot, p = q // per2, q % per2
            else:
                slot, p = 3, q - pairs
            back = LANES - (16 * p + lo) + (0 if odd else half_lanes)
            for k in range(ext[2][1] // 8):
                rows = pl.ds(8 * k, 8)
                own = p2[pair, rows, :]
                own = pltpu.roll(own, half_lanes, 1) if odd else own
                low = pltpu.roll(hzl[0, slot, rows, :], back % LANES, 1)
                high = pltpu.roll(hzl[1, slot, rows, :], back % LANES, 1)
                v = jnp.where(lane8 < 3 * half_lanes // 2, high, low)
                g[at(e + lo, k, 0, 0)] = jnp.where(lane8 < half_lanes, own, v)

    def ext_sweep(mode, l, src, dst, size, reach):
        nt, origin = ext[l][2], ext[l][3]
        nx, ny, _ = dims[l]
        g = b[f"G{l}"]
        first = OWN - reach[0]
        rows = 8 * -(-(ny + sum(reach)) // 8)

        def some(i, count):
            for q in range(count):
                p = i + q
                new = stencil(mode, l, src, g, p, (p - 1, p + 1), first, rows, nt, True)
                for t, value in enumerate(new):
                    dst[p, t, pl.ds(first, rows), :] = value

        groups(origin - reach[0], origin + nx + reach[1], size, some)

    def spread_rows(q, v, j, c0, t):
        c, n = q[at(j, 0, t, OWN + c0)], q[at(j, 0, t, OWN + c0 + 1)]
        return c, 0.5 * (c + n)

    st, sg = b["stats"], [b[f"sums{a}"] for a in range(3)]

    def spread_sums(a):
        return [
            copy(st.at[a], sg[a].at[j], tuple(j if i == a else 0 for i in range(3)))
            for j in range(1, counts[a])
        ]

    def gather_sums(a, copies):
        wait(copies)
        total = st[a]
        for j in range(1, counts[a]):
            total = total + sg[a][j]
        if a < 2:
            st[a + 1] = total
        return total

    def fold(ref):
        def step(p, totals):
            totals = list(totals)
            for q in range(2):
                for k in range(nb0):
                    for t in range(nt0):
                        totals[(2 * k + t) % 4] += ref[at(2 * p + q, k, t)]
            return tuple(totals)

        t = lax.fori_loop(0, x0 // 2, step, (zero8,) * 4)
        return (t[0] + t[1]) + (t[2] + t[3])

    a1, b1, g1 = b["A1"], b["B1"], b["G1"]
    a2, b2, g2 = b["A2"], b["B2"], b["G2"]

    with jax.named_scope("clear"):

        def clear0(i, _):
            for ref in (u, a0, b0):
                for t in range(nt0):
                    ref[i, t, pl.ds(0, OWN), :] = zero8
                    ref[i, t, pl.ds(OWN + y0, OWN), :] = zero8
            return 0

        lax.fori_loop(0, x0, clear0, 0)
        for l in (1, 2):
            ex, ey, tiles, _ = ext[l]
            refs = [b[f"{name}{l}"] for name in "GAB"]

            def clear(i, _, refs=refs, ey=ey, tiles=tiles):
                for ref in refs:
                    for k in range(ey // 8):
                        for t in range(tiles):
                            ref[at(i, k, t, 0)] = zero8
                return 0

            lax.fori_loop(0, ex, clear, 0)
            for side in range(2):
                for slot in range(b[f"hz{l}"].shape[1]):
                    for k in range(ey // 8):
                        b[f"hz{l}"][side, slot, pl.ds(8 * k, 8), :] = zero8
        for p in range(b["P2"].shape[0]):
            for k in range(ext[2][1] // 8):
                b["P2"][p, pl.ds(8 * k, 8), :] = zero8
    with jax.named_scope("loadu"):
        loads[0].wait()
        loads[1].wait()
    with jax.named_scope("packu"):

        def pack_some(i, count):
            for q in range(count):
                pack_z(b["zp"].at[0], i + q, u)

        groups(0, x0, 8, pack_some)
    with jax.named_scope("sumu"):
        st[0, 0] = fold(u)
    with jax.named_scope("barrier"):
        pl.semaphore_wait(barrier, len(offsets))
    send_x, send_y, send_z = exchange(0, u)
    moving = send_x() + send_y() + send_z()
    with jax.named_scope("sumf"):
        loads[2].wait()
        loads[3].wait()
        st[0, 1] = fold(f)
    sums = spread_sums(0)
    faces = b["yp"]
    moving = sweep(0, moving, u, a0, exchange(1, a0, faces.at[1]))
    gather_sums(0, sums)
    sums = spread_sums(1)
    moving = sweep(1, moving, a0, b0, exchange(2, b0, faces.at[0]))
    gather_sums(1, sums)
    sums = spread_sums(2)
    moving = sweep(2, moving, b0, d0, defect_exchange(3, d0), mode="defect")
    with jax.named_scope("step3"):

        def step3(i, count):
            for q in range(count):
                for t in range(nt0):
                    a0[i + q, t, own0, :] = b0[i + q, t, own0, :] + W * d0[i + q, t, own0, :]
            for q in range(count):
                pack_z(b["zp"].at[0], i + q, a0)

        groups(0, x0, 8, step3)
    send_x, send_y, send_z = exchange(4, a0)
    moving3 = send_x() + send_y() + send_z()
    total = gather_sums(2, sums)
    mean_u = jnp.sum(total[0]) * (1.0 / cells)
    mean_f = jnp.sum(total[1]) * (1.0 / cells)
    wait(moving)

    with jax.named_scope("restrict0"):
        lane = lax.broadcasted_iota(jnp.int32, (y0 + 8, LANES), 1)
        moved = pltpu.roll(b["rw"][...], 1, 1)
        rim = jnp.where(lane == last, moved, b["rz"][...])
        b["m"][...] = dot_split(rim, restrict_matrix(LANES, LANES, x1, last, 2))
        m = b["m"]
        v = 0.25 * (m[pl.ds(OWN - 1, y1, stride=2), :] + m[pl.ds(OWN + 1, y1, stride=2), :])
        b["n"][...] = 0.25 * (v + 0.5 * m[pl.ds(OWN, y1, stride=2), :])
        restrict_planes(d0, x0, 0, 0, nb0 + 1, nt0, b["T0"])
        w = restrict_matrix(z0, LANES, z1)
        o1, own1 = ext[1][3], pl.ds(OWN, y1)
        multiply(b["T0"], g1, w, 0, x1, 8, pl.ds(0, y1), o1, own1)

        def finish(i, count):
            for q in range(count):
                for k in range(y1 // 8):
                    col = pltpu.roll(b["n"][pl.ds(8 * k, 8), :], turn(2 * LANES - (i + q)), 1)
                    where = at(i + q + o1, k, 0)
                    g1[where] = g1[where] + jnp.where(lane8 == 0, col, 0.0) - mean_f

        groups(0, x1, 8, finish)
    moving = halo_send(1, g1.at[:, 0], x1, HALO1, HALO1, True)
    with jax.named_scope("pack1"):
        halo_pack1()
    moving = moving + halo_send(1, g1.at[:, 0], x1, HALO1, HALO1, False)
    sweep(4, moving3, a0, b0)
    wait(moving)
    with jax.named_scope("unpack1"):
        halo_unpack1()
    with jax.named_scope("first1"):
        ext_sweep("first", 1, g1, b1, 13, (3, 4))
    with jax.named_scope("defect1"):
        ext_sweep("defect", 1, b1, a1, 19, (1, 0))
    with jax.named_scope("restrict1"):
        t1 = b["T1"]
        blocks1 = -(-(y1 + 1) // 8)
        restrict_planes(a1, o1 - 1, o1, OWN - 1, blocks1, 2, t1)
        w = restrict_matrix(2 * LANES, LANES // 2, z2, 2 * LANES - 1)
        none = jnp.zeros_like(w)
        w = jnp.concatenate([jnp.concatenate([w, none], 1), jnp.concatenate([none, w], 1)], 0)
        paired = []
        for half in range(2):
            for t in range(2):
                v = [t1[2 * p + half, t] for p in range(pairs)]
                paired.append(jnp.concatenate(v, 0))
        v = dot_split(jnp.concatenate(paired, 1), w).reshape(pairs, y2, LANES)
        b["P2"][pl.ds(low_pairs, pairs), pl.ds(OWN, y2), :] = v
    depth2 = (low_pairs, high_pairs)
    moving = halo_send(2, b["P2"], pairs, depth2, HALO2, True)
    with jax.named_scope("pack2"):
        halo_pack2()
    moving = moving + halo_send(2, b["P2"], pairs, depth2, HALO2, False)
    wait(moving)
    with jax.named_scope("unpack2"):
        halo_unpack2()
    with jax.named_scope("sweeps2"):
        v, w2 = a2, b2
        reach = [(k + 2, k + 3) for k in range(COARSE_SWEEPS - 1)][::-1]
        ext_sweep("first", 2, g2, v, 27, reach[0])
        for k in range(1, COARSE_SWEEPS - 1):
            ext_sweep("relax", 2, v, w2, 27, reach[k])
            v, w2 = w2, v
    with jax.named_scope("prolong1"):
        o2 = ext[2][3]
        q1, v1 = b["Q1"], b["V1"]
        w = prolong_matrix(LANES, 2 * LANES, z1, True)
        multiply(v, q1, w, o2 - 2, x2 + 5, x2 + 5, pl.ds(0, ext[2][1]), 0, pl.ds(0, ext[2][1]))

        def spread1(i, count):
            for q in range(count):
                for t in range(2):
                    for c0 in range(-2, (y1 + 3) // 2, 8):
                        even, odd = spread_rows(q1, v1, i + q, c0, t)
                        v1[i + q, t, pl.ds(OWN + 2 * c0, 8, stride=2), :] = even
                        v1[i + q, t, pl.ds(OWN + 2 * c0 + 1, 8, stride=2), :] = odd

        groups(o2 - 2, o2 + x2 + 3, 7, spread1)

        def add1(i, count):
            for q in range(count):
                j = i + q
                rows = pl.ds(OWN - 3, 8 * -(-(y1 + 7) // 8))
                for t in range(2):
                    c, n = v1[j + o2, t, rows, :], v1[j + 1 + o2, t, rows, :]
                    even, odd = 2 * j + o1, 2 * j + o1 + 1
                    b1[even, t, rows, :] = b1[even, t, rows, :] + c
                    b1[odd, t, rows, :] = b1[odd, t, rows, :] + 0.5 * (c + n)

        groups(-2, x2 + 2, 4, add1)
    with jax.named_scope("post1"):
        ext_sweep("relax", 1, b1, a1, 19, (2, 3))
        ext_sweep("relax", 1, a1, b1, 18, (1, 2))
    keep = 1.0 - relax_weight
    coarse = [b[name] for name in ("CA", "CB", "CC")]
    fine = [u, d0, a0]

    def spread(a, bb, c):
        be, bo = bb[-1] + bb[1], bb[0] + bb[1]
        ce, co = c[0] + c[0] + (c[-1] + c[1]), c[0] + c[1]
        e0 = a[0] + (bb[0] + 0.5 * be) + ce
        o0 = 0.5 * ((a[0] + a[1]) + (c[-1] + c[2])) + (bo + 1.5 * co)
        return e0, o0, (bb[0] + ce, 0.5 * bo + 2.0 * co), (c[0], 0.5 * co)

    with jax.named_scope("tailz"):
        shift = mean_u + 4.0 * W * mean_f
        w = hat_matrices(2 * LANES, z0)
        chunk, rows = 5, pl.ds(OWN - 1, y1 + 8)

        def tail_z(k, _):
            i = k * chunk
            v = dot_split(planes_of(b1, i + o1 - 1, chunk, rows), w)
            for t in range(nt0):
                z = [v[:, z0 * n + LANES * t : z0 * n + LANES * t + LANES] for n in range(3)]
                ca = keep**2 * z[0] + (2.0 * keep * W) * z[1] + W**2 * z[2] - shift
                cb = (2.0 * keep * W) * z[0] + (2.0 * W**2) * z[1]
                for ref, value in zip(coarse, (ca, cb, W**2 * z[0])):
                    ref[pl.ds(i, chunk), t, rows, :] = value.reshape(chunk, -1, LANES)
            return 0

        assert (x1 + 3) % chunk == 0
        lax.fori_loop(0, (x1 + 3) // chunk, tail_z, 0)
    with jax.named_scope("taily"):

        def tail_y(i, count):
            for q in range(count):
                for t in range(nt0):
                    near = [
                        {d: ref[i + q, t, pl.ds(OWN + d, y1), :] for d in (-1, 0, 1, 2)}
                        for ref in coarse
                    ]
                    e0, o0, one, two = spread(*near)
                    for ref, even, odd in ((fine[0], e0, o0), (fine[1], *one), (fine[2], *two)):
                        ref[i + q, t, pl.ds(0, y1, stride=2), :] = even
                        ref[i + q, t, pl.ds(1, y1, stride=2), :] = odd

        groups(0, x1 + 3, 5, tail_y)
    with jax.named_scope("tailx"):
        rows0 = pl.ds(0, y0)

        def tail_x(i, count):
            for q in range(count):
                j = i + q
                for t in range(nt0):
                    near = [
                        {d: ref[j + 1 + d, t, rows0, :] for d in (-1, 0, 1, 2)} for ref in fine
                    ]
                    e0, o0, _, _ = spread(*near)
                    lanes = pl.ds(LANES * t, LANES)
                    out[2 * j, :, lanes] = b0[2 * j, t, own0, :] + e0
                    out[2 * j + 1, :, lanes] = b0[2 * j + 1, t, own0, :] + o0

        groups(0, x1, 4, tail_x)


def solution(mesh):
    counts = tuple(mesh.shape[a] for a in AXES)

    def shards(right_side, initial_guess):
        shape = right_side.shape
        dims = tuple(tuple(n >> l for n in shape) for l in range(3))
        cells = float(right_side.size)
        for n in counts:
            cells *= n
        bufs = buffers(dims, counts)
        messages = 2 * 8 + 2 * 6 + 9 + 2 * 26 + sum(counts) - 3
        return pl.pallas_call(
            functools.partial(kernel, dims, counts, tuple(bufs), cells),
            out_shape=jax.ShapeDtypeStruct(shape, jnp.float32),
            in_specs=[pl.BlockSpec(memory_space=pl.ANY)] * 2,
            out_specs=pl.BlockSpec(memory_space=pltpu.VMEM),
            scratch_shapes=list(bufs.values())
            + [pltpu.SemaphoreType.DMA((n,)) for n in (messages, messages, 4)],
            compiler_params=pltpu.CompilerParams(
                collective_id=0, has_side_effects=True, vmem_limit_bytes=56 * 1024 * 1024
            ),
        )(initial_guess, right_side)

    placed = (P(*AXES), P(*AXES))
    return jax.shard_map(
        shards, mesh=mesh, in_specs=placed, out_specs=P(*AXES), check_vma=False
    )
```

```python
import functools
import itertools

import jax
import jax.numpy as jnp
from jax import lax
from jax.experimental import pallas as pl
from jax.experimental.pallas import tpu as pltpu
from jax.sharding import PartitionSpec as P

COARSE_SWEEPS = 6
LANES = 128
AXES = ("gx", "gy", "gz")
relax_weight = 0.8
W = relax_weight / 6.0

SWEEP_PLANES = 10
FIX_PLANES = 12

HALO1 = (4, 5)
HALO2 = (COARSE_SWEEPS + 1, COARSE_SWEEPS + 2)


def dot_split(a, w):
    hi = a.astype(jnp.bfloat16)
    mid = (a - hi.astype(jnp.float32)).astype(jnp.bfloat16)
    rows = a.shape[0]
    v = jnp.dot(jnp.concatenate([hi, mid], 0), w, preferred_element_type=jnp.float32)
    return v[:rows] + v[rows:]


def iotas(shape):
    return (
        lax.broadcasted_iota(jnp.int32, shape, 0),
        lax.broadcasted_iota(jnp.int32, shape, 1),
    )


def restrict_matrix(rows, cols, count, wrap=None, step=1):
    r, c = iotas((rows, cols))
    d = jnp.abs(r - 2 * step * c)
    w = jnp.where(d == 0, 0.5, 0.0) + jnp.where(d == step, 0.25, 0.0)
    w = jnp.where((c < count) & (r < 2 * step * count), w, 0.0)
    if wrap is not None:
        w = w + jnp.where((r == wrap) & (c == 0), 0.25, 0.0)
    return w.astype(jnp.bfloat16)


def prolong_matrix(rows, cols, fine, wrapped):
    r, c = iotas((rows, cols))
    if wrapped:
        r = jnp.where(r < 3 * rows // 4, r, r - rows)
        c = jnp.where(c < 3 * cols // 4, c, c - cols)
    d = jnp.abs(c - 2 * r)
    w = jnp.where(d == 0, 1.0, 0.0) + jnp.where(d == 1, 0.5, 0.0)
    return w.astype(jnp.bfloat16)


def hat_matrices(rows, cols):
    r, c = iotas((rows, cols))
    d = jnp.abs(c - 2 * jnp.where(r < 3 * rows // 4, r, r - rows))
    parts = []
    for row in ((1.0, 0.5), (1.0, 1.0, 0.5), (2.0, 1.5, 1.0, 0.5)):
        w = jnp.zeros((rows, cols), jnp.float32)
        for k, value in enumerate(row):
            w = w + jnp.where(d == k, value, 0.0)
        parts.append(w.astype(jnp.bfloat16))
    return jnp.concatenate(parts, 1)


def turn(by):
    return by % LANES if isinstance(by, int) else lax.rem(by, LANES)


OWN = 8


def extended(dims):
    (x1, y1, _), (x2, y2, _) = dims[1], dims[2]
    up = lambda n: -(-n // 8) * 8
    return (
        None,
        (x1 + sum(HALO1), up(y1 + OWN + HALO1[1] + 9), 2, HALO1[0]),
        (x2 + sum(HALO2), up(y2 + OWN + HALO2[1] + 4), 1, HALO2[0]),
    )


def buffers(dims, counts):
    (x, y, z), (x1, y1, _), (x2, y2, _) = dims
    ext = extended(dims)
    nt = z // LANES
    out = {}
    for name in ("u", "f", "A0", "B0"):
        out[name] = (x, nt, y + 2 * OWN, LANES)
    out["D0"] = (x, nt, y + OWN, LANES)
    out["rx"] = (nt, y + OWN, LANES)
    out["ry"] = (nt, x + OWN, LANES)
    out["e"] = (x1 + y1, LANES)
    out["yp"] = (2, 2, nt, x, LANES)
    out["zp"] = (2, y, LANES)
    out["zh"] = (y, LANES)
    out["hx"] = (5, 2, nt, y, LANES)
    out["hy"] = (5, 2, nt, x, LANES)
    out["hz"] = (5, 2, y, LANES)
    out["rz"] = (y + OWN, LANES)
    out["rw"] = (y + OWN, LANES)
    out["m"] = (y + OWN, LANES)
    out["n"] = (y // 2, LANES)
    out["S"] = (4, nt, y + OWN, LANES)
    out["T0"] = (x1, nt, y1, LANES)
    out["T1"] = (x2, 2, y2, LANES)
    for l, ny in ((1, y1), (2, y2)):
        ex, ey, tiles, _ = ext[l]
        for name in "GAB":
            out[f"{name}{l}"] = (ex, tiles, ey, LANES)
        packs = 2 if l == 2 else -(-x1 * sum(HALO1) // LANES)
        out[f"zp{l}"] = (packs, ny, LANES)
        out[f"hz{l}"] = (2, packs + 2, ey, LANES)
    out["P2"] = (x2 // 2 + -(-HALO2[0] // 2) + -(-HALO2[1] // 2), ext[2][1], LANES)
    out["Q1"] = (ext[2][0], 2, ext[2][1], LANES)
    out["V1"] = (ext[2][0], 2, ext[1][1] + 8, LANES)
    for name in ("CA", "CB", "CC"):
        out[name] = (x1 + 3, nt, ext[1][1], LANES)
    out["stats"] = (3, 2, 8, LANES)
    for a in range(3):
        out[f"sums{a}"] = (counts[a], 2, 8, LANES)
    return {k: pltpu.VMEM(v, jnp.float32) for k, v in out.items()}


def kernel(dims, counts, names, cells, u_far, f_far, out, *scratch):
    b = dict(zip(names, scratch[:-3]))
    send_sem, recv_sem, load_sem = scratch[-3:]
    u, f, a0, b0, d0 = b["u"], b["f"], b["A0"], b["B0"], b["D0"]
    loads = []
    for n, (far, near) in enumerate(((u_far, u), (f_far, f))):
        for t in range(2):
            lanes = pl.ds(LANES * t, LANES)
            own = near.at[:, t, pl.ds(OWN, dims[0][1]), :]
            c = pltpu.make_async_copy(far.at[:, :, lanes], own, load_sem.at[2 * n + t])
            c.start()
            loads.append(c)
    here = {a: lax.axis_index(a) for a in AXES}
    serial = itertools.count()
    ext = extended(dims)
    x0, y0, z0 = dims[0]
    x1, y1, z1 = dims[1]
    x2, y2, z2 = dims[2]
    nb0, nt0 = y0 // 8, z0 // LANES
    assert 2 * x0 == LANES and z1 == LANES and 2 * z2 == LANES
    assert nt0 == 2 and y2 % 8 == 0

    def device(offset):
        return tuple(lax.rem(here[a] + (o % n), n) for a, o, n in zip(AXES, offset, counts))

    def copy(src, dst, offset):
        k = next(serial)
        c = pltpu.make_async_remote_copy(
            src_ref=src,
            dst_ref=dst,
            send_sem=send_sem.at[k],
            recv_sem=recv_sem.at[k],
            device_id=device(offset),
            device_id_type=pl.DeviceIdType.MESH,
        )
        c.start()
        return c

    def wait(copies):
        with jax.named_scope("wait"):
            for c in copies:
                c.wait()

    around = [o for o in itertools.product((-1, 0, 1), repeat=3) if any(o)]
    offsets = list(around)
    for a in range(3):
        for j in range(2, counts[a] - 1):
            offsets.append(tuple(j if i == a else 0 for i in range(3)))
    barrier = pltpu.get_barrier_semaphore()
    for o in offsets:
        pl.semaphore_signal(
            barrier, inc=1, device_id=device(o), device_id_type=pl.DeviceIdType.MESH
        )

    row8 = lax.broadcasted_iota(jnp.int32, (8, LANES), 0)
    lane8 = lax.broadcasted_iota(jnp.int32, (8, LANES), 1)
    zero8 = jnp.zeros((8, LANES), jnp.float32)

    def at(i, k, t, first=OWN):
        return i, t, pl.ds(first + 8 * k, 8), slice(None)

    def groups(lo, hi, size, body):
        steps = (hi - lo) // size

        def step(p, _):
            body(lo + size * p, size)
            return 0

        if steps > 1:
            lax.fori_loop(0, steps, step, 0)
        elif steps:
            body(lo, size)
        if (hi - lo) % size:
            body(lo + size * steps, (hi - lo) % size)

    def lanes_of(rows):
        return lax.broadcasted_iota(jnp.int32, (rows, LANES), 1)

    def stencil(mode, l, src, g, i, near, first, rows, nt, z_wrap, shift=None):
        scale = 0.25**l
        lane = lanes_of(rows)
        here, above, below = (pl.ds(first + d, rows) for d in (0, -1, 1))
        c = [src[i, t, here, :] for t in range(nt)]
        left = [pltpu.roll(v, 1, 1) for v in c]
        right = [pltpu.roll(v, LANES - 1, 1) for v in c]
        new = []
        for t in range(nt):
            v = c[t]
            s = src[i, t, above, :] + src[i, t, below, :]
            for j in near:
                s = s + src[j, t, here, :]
            if z_wrap and nt == 1:
                s = s + (left[t] + right[t])
            else:
                before = left[t - 1] if t or z_wrap else 0.0
                after = right[(t + 1) % nt] if t < nt - 1 or z_wrap else 0.0
                z = jnp.where(lane == 0, before, left[t])
                s = s + (z + jnp.where(lane == LANES - 1, after, right[t]))
            if mode == "first":
                z = W / scale
                value = (W * z) * s + (W * (1.5 * z + 1.0 / scale)) * v
            elif mode == "defect":
                value = s - 6.0 * v
                value = g[i, t, here, :] + (value if l == 0 else scale * value)
            else:
                gv = g[i, t, here, :]
                value = s + 1.5 * v
                value = W * (value + (gv if l == 0 else (1.0 / scale) * gv))
                if shift is not None:
                    value = value - shift
            new.append(value)
        return new

    zh = b["zh"]
    last = LANES - 1

    def pack_z(zp, i, ref):
        lane = lanes_of(y0)
        both = jnp.where(lane == last, ref[i, nt0 - 1, own0, :], ref[i, 0, own0, :])
        moved = pltpu.roll(both, turn(2 * i + 1), 1)
        pltpu.store(zp, moved, mask=(lane == 2 * i) | (lane == 2 * i + 1))

    def pack_rows(yp, i, new):
        for side, r in ((0, 0), (1, y0 - 1)):
            for t in range(nt0):
                yp[side, t, pl.ds(i, 1), :] = new[t][r : r + 1]

    own0 = pl.ds(OWN, y0)

    def exchange(r, src, faces=None):
        hx, hy, hz = b["hx"].at[r], b["hy"].at[r], b["hz"].at[r]
        zp = b["zp"].at[r % 2]

        def send_x():
            return [
                copy(src.at[x0 - 1, :, own0], hx.at[0], (1, 0, 0)),
                copy(src.at[0, :, own0], hx.at[1], (-1, 0, 0)),
            ]

        def send_y():
            if faces is not None:
                return [
                    copy(faces.at[1], hy.at[0], (0, 1, 0)),
                    copy(faces.at[0], hy.at[1], (0, -1, 0)),
                ]
            started = []
            for t in range(nt0):
                started.append(copy(src.at[:, t, OWN + y0 - 1], hy.at[0, t], (0, 1, 0)))
                started.append(copy(src.at[:, t, OWN], hy.at[1, t], (0, -1, 0)))
            return started

        def send_z():
            return [
                copy(zp, hz.at[0], (0, 0, 1)),
                copy(zp, hz.at[1], (0, 0, -1)),
            ]

        return send_x, send_y, send_z

    def defect_exchange(r, d):
        rz, rw = b["rz"], b["rw"]
        yp, zp = b["yp"].at[r % 2], b["zp"].at[r % 2]

        def send_x():
            return [copy(d.at[x0 - 1, :, own0], b["rx"].at[:, own0], (1, 0, 0))]

        def send_y():
            started = []
            for t in range(nt0):
                ry = b["ry"].at[t]
                started.append(copy(yp.at[1, t, x0 - 1], ry.at[OWN - 1], (1, 1, 0)))
                started.append(copy(yp.at[1, t], ry.at[pl.ds(OWN, x0)], (0, 1, 0)))
            return started

        def send_z():
            end, before = zp.at[pl.ds(y0 - 1, 1)], pl.ds(OWN - 1, 1)
            return [
                copy(end, rw.at[before], (1, 1, 1)),
                copy(zp, rw.at[own0], (1, 0, 1)),
                copy(end, rz.at[before], (0, 1, 1)),
                copy(zp, rz.at[own0], (0, 0, 1)),
            ]

        return send_x, send_y, send_z

    def sweep(r, moving, src, dst, onward=None, mode="relax", shift=None):
        hx, hy, hz = b["hx"].at[r], b["hy"].at[r], b["hz"].at[r]
        yp, zp = b["yp"].at[(r + 1) % 2], b["zp"].at[(r + 1) % 2]
        gain = 1.0 if mode == "defect" else W
        packed = onward is not None

        def plane(i, near):
            new = stencil(mode, 0, src, f, i, near, OWN, y0, nt0, False, shift)
            for t, value in enumerate(new):
                dst[i, t, own0, :] = value
            if packed:
                pack_rows(yp, i, new)

        def some(i, count):
            for q in range(count):
                plane(i + q, (i + q - 1, i + q + 1))
            if packed:
                for q in range(count):
                    pack_z(zp, i + q - 2, dst)

        with jax.named_scope("inner"):
            plane(0, (1,))
            plane(x0 - 1, (x0 - 2,))
            plane(1, (0, 2))
            plane(2, (1, 3))
            groups(3, x0 - 1, SWEEP_PLANES, some)
            if packed:
                pack_z(zp, x0 - 3, dst)
                pack_z(zp, x0 - 2, dst)
        wait(moving() if callable(moving) else moving)
        odd = lane8 % 2 == 1
        for k in range(nb0):
            rows = pl.ds(8 * k, 8)
            before = pltpu.roll(hz[0, rows, :], 1, 1)
            after = pltpu.roll(hz[1, rows, :], LANES - 1, 1)
            zh[rows, :] = gain * jnp.where(odd, before, after)

        def fix(i, size, beyond=None):
            done = []
            lane = lanes_of(y0)
            for q in range(size):
                p = i + q
                halo = pltpu.roll(zh[...], turn(2 * LANES - 2 * p - 1), 1)
                for t in range(nt0):
                    v = dst[p, t, own0, :]
                    if beyond is not None:
                        v = v + gain * beyond[t]
                    if t == 0:
                        v = v + jnp.where(lane == 0, halo, 0.0)
                    if t == nt0 - 1:
                        v = v + jnp.where(lane == last, halo, 0.0)
                    low, high = (gain * hy[s, t, pl.ds(p, 1), :] for s in range(2))
                    low = v[:8] + jnp.where(row8 == 0, low, 0.0)
                    high = v[y0 - 8 :] + jnp.where(row8 == 7, high, 0.0)
                    done.append((p, t, OWN, low))
                    done.append((p, t, OWN + 8, v[8 : y0 - 8]))
                    done.append((p, t, OWN + y0 - 8, high))
            for p, t, start, v in done:
                dst[p, t, pl.ds(start, v.shape[0]), :] = v

        with jax.named_scope("ends"):
            fix(0, 1, hx.at[0])
            fix(x0 - 1, 1, hx.at[1])
        if not packed:
            with jax.named_scope("fix"):
                groups(1, x0 - 1, FIX_PLANES, fix)
            return []
        started = onward[0]()
        with jax.named_scope("yface"):
            for side, r0 in ((0, 0), (1, y0 - 1)):
                line = jnp.broadcast_to(zh[pl.ds(r0, 1), :], (8, LANES))
                for j in range(x0 // 8):
                    slot = 2 * (8 * j + row8)
                    low = jnp.sum(jnp.where(lane8 == slot + 1, line, 0.0), 1, keepdims=True)
                    high = jnp.sum(jnp.where(lane8 == slot, line, 0.0), 1, keepdims=True)
                    for t in range(nt0):
                        rows = (side, t, pl.ds(8 * j, 8), slice(None))
                        v = yp[rows] + gain * hy[rows]
                        if t == 0:
                            v = v + jnp.where(lane8 == 0, low, 0.0)
                        if t == nt0 - 1:
                            v = v + jnp.where(lane8 == last, high, 0.0)
                        yp[rows] = v
                for i in (0, x0 - 1):
                    for t in range(nt0):
                        yp[side, t, pl.ds(i, 1), :] = dst[i, t, pl.ds(OWN + r0, 1), :]
        started = started + onward[1]()
        with jax.named_scope("zface"):
            for k in range(nb0):
                v = zp[pl.ds(8 * k, 8), :] + zh[pl.ds(8 * k, 8), :]
                for side, kk, rr in ((0, 0, 0), (1, nb0 - 1, 7)):
                    if k == kk:
                        total = zero8
                        for j in range(x0 // 8):
                            slot = 2 * (8 * j + row8)
                            low = hy[side, 0, pl.ds(8 * j, 8), :][:, :1]
                            high = hy[side, nt0 - 1, pl.ds(8 * j, 8), :][:, last:]
                            total = total + jnp.where(lane8 == slot + 1, low, 0.0)
                            total = total + jnp.where(lane8 == slot, high, 0.0)
                        total = gain * jnp.sum(total, 0, keepdims=True)
                        v = v + jnp.where(row8 == rr, total, 0.0)
                zp[pl.ds(8 * k, 8), :] = v
            pack_z(zp, 0, dst)
            pack_z(zp, x0 - 1, dst)
        started = started + onward[2]()
        with jax.named_scope("fix"):
            groups(1, x0 - 1, FIX_PLANES, fix)
        return started

    def restrict_xy(d, low, middle, j, u_slot, first, nb, nt, dst):
        s = b["S"].at[u_slot]
        n = dst.shape[2]
        rows = pl.ds(first, 8 * nb)
        for t in range(nt):
            v = d[middle + 1, t, rows, :]
            v = 0.25 * (v if low is None else v + d[low, t, rows, :])
            s[t, rows, :] = v + 0.5 * d[middle, t, rows, :]
        for t in range(nt):
            around = s[t, pl.ds(OWN - 1, n, stride=2), :] + s[t, pl.ds(OWN + 1, n, stride=2), :]
            dst[j, t] = 0.25 * around + 0.5 * s[t, pl.ds(OWN, n, stride=2), :]

    def restrict_planes(d, before, origin, first, nb, nt, dst):
        restrict_xy(d, before, origin, 0, 0, first, nb, nt, dst)
        for j in range(1, 4):
            restrict_xy(d, origin + 2 * j - 1, origin + 2 * j, j, j, first, nb, nt, dst)

        def some(p, _):
            for q in range(4):
                j = 4 * p + q
                restrict_xy(d, origin + 2 * j - 1, origin + 2 * j, j, q, first, nb, nt, dst)
            return 0

        lax.fori_loop(1, dst.shape[0] // 4, some, 0)

    def planes_of(src, i, chunk, rows):
        parts = [src[pl.ds(i, chunk), t, rows, :] for t in range(src.shape[1])]
        parts = [v.reshape(chunk * v.shape[1], LANES) for v in parts]
        return jnp.concatenate(parts, 1) if len(parts) > 1 else parts[0]

    def multiply(src, dst, w, first, count, chunk, rows, shift, to_rows, less=None):
        tiles = w.shape[1] // LANES

        def step(k, _):
            i = first + k * chunk
            v = dot_split(planes_of(src, i, chunk, rows), w)
            if less is not None:
                v = v - less
            for t in range(tiles):
                part = v[:, LANES * t : LANES * t + LANES]
                dst[pl.ds(i + shift, chunk), t, to_rows, :] = part.reshape(chunk, -1, LANES)
            return 0

        if count == chunk:
            step(0, 0)
        else:
            lax.fori_loop(0, count // chunk, step, 0)

    def region(o, start, n, depth):
        lo, hi = depth
        if o == 1:
            return pl.ds(start + n - lo, lo), pl.ds(start - lo, lo)
        if o == -1:
            return pl.ds(start, hi), pl.ds(start + n, hi)
        return pl.ds(start, n), pl.ds(start, n)

    def halo_send(l, g, nx, depth_x, depth):
        zpl, hzl = b[f"zp{l}"], b[f"hz{l}"]
        ny = dims[l][1]
        started = []
        for o in sorted(around, key=lambda v: -sum(map(abs, v))):
            sx, dx = region(o[0], depth_x[0], nx, depth_x)
            sy, dy = region(o[1], OWN, ny, depth)
            if o[2] == 0:
                started.append(copy(g.at[sx, sy], g.at[dx, dy], o))
            else:
                side = 0 if o[2] == 1 else 1
                packs = zpl.shape[0]
                half = {0: (0, packs), 1: (packs - 1, 1), -1: (0, 1)}[o[0]]
                slot = {0: 0, 1: packs, -1: packs + 1}[o[0]]
                sy = pl.ds(sy.start - OWN, sy.size)
                source = zpl.at[pl.ds(*half), sy]
                started.append(copy(source, hzl.at[side, pl.ds(slot, half[1]), dy], o))
        return started

    def merge_sides(l, left):
        hzl = b[f"hz{l}"]
        for slot in range(hzl.shape[1]):
            for k in range(ext[l][1] // 8):
                rows = pl.ds(8 * k, 8)
                v = jnp.where(left, hzl[0, slot, rows, :], hzl[1, slot, rows, :])
                hzl[0, slot, rows, :] = v

    def halo_pack1():
        g, zpl = b["G1"], b["zp1"]
        lo, hi = HALO1
        width, packs = lo + hi, zpl.shape[0]
        per = -(-x1 // packs)
        for half in range(packs):
            total = [zero8] * (y1 // 8)
            for p in range(min(per, x1 - half * per)):
                first = width * p
                mask = (lane8 >= first) & (lane8 < first + width)
                for k in range(y1 // 8):
                    v = pltpu.roll(g[at(lo + half * per + p, k, 0)], first + lo, 1)
                    total[k] = jnp.where(mask, v, total[k])
            for k in range(y1 // 8):
                zpl[half, pl.ds(8 * k, 8), :] = total[k]

    def halo_unpack1():
        g, hzl = b["G1"], b["hz1"]
        lo, hi = HALO1
        width, packs = lo + hi, hzl.shape[1] - 2
        per = -(-x1 // packs)
        assert per * width <= LANES and hi <= per and lo <= x1 - (packs - 1) * per
        left = lane8 < lo
        for p in range(1, per):
            left = left | ((lane8 >= width * p) & (lane8 < width * p + lo))
        merge_sides(1, left)
        for e in range(-lo, x1 + hi):
            if e < 0:
                slot, p = packs, x1 + e - (packs - 1) * per
            elif e < x1:
                slot, p = e // per, e % per
            else:
                slot, p = packs + 1, e - x1
            back = LANES - (width * p + lo)
            for k in range(ext[1][1] // 8):
                v = hzl[0, slot, pl.ds(8 * k, 8), :]
                g[at(e + lo, k, 1, 0)] = pltpu.roll(v, back % LANES, 1)

    low_pairs, high_pairs = -(-HALO2[0] // 2), -(-HALO2[1] // 2)
    pairs, per2 = x2 // 2, x2 // 4
    assert sum(HALO2) <= 16 and per2 <= 4 and max(low_pairs, high_pairs) <= per2

    def halo_pack2():
        p2, zpl = b["P2"], b["zp2"]
        lo, hi = HALO2
        for half in range(2):
            total = [zero8] * (y2 // 8)
            for p in range(per2):
                first = lane8 % (LANES // 2) - 16 * p
                mask = (first >= 0) & (first < lo + hi)
                for k in range(y2 // 8):
                    v = p2[low_pairs + half * per2 + p, pl.ds(OWN + 8 * k, 8), :]
                    v = pltpu.roll(v, 16 * p + lo, 1)
                    total[k] = jnp.where(mask, v, total[k])
            for k in range(y2 // 8):
                zpl[half, pl.ds(8 * k, 8), :] = total[k]

    def halo_unpack2():
        g, p2, hzl = b["G2"], b["P2"], b["hz2"]
        lo, hi = HALO2
        half_lanes = LANES // 2
        for e in range(-lo, x2 + hi):
            pair, odd = (e + 2 * low_pairs) // 2, e % 2
            q = pair - low_pairs
            if q < 0:
                slot, p = 2, q + per2
            elif q < pairs:
                slot, p = q // per2, q % per2
            else:
                slot, p = 3, q - pairs
            back = LANES - (16 * p + lo) + (0 if odd else half_lanes)
            for k in range(ext[2][1] // 8):
                rows = pl.ds(8 * k, 8)
                own = p2[pair, rows, :]
                own = pltpu.roll(own, half_lanes, 1) if odd else own
                low = pltpu.roll(hzl[0, slot, rows, :], back % LANES, 1)
                high = pltpu.roll(hzl[1, slot, rows, :], back % LANES, 1)
                v = jnp.where(lane8 < 3 * half_lanes // 2, high, low)
                g[at(e + lo, k, 0, 0)] = jnp.where(lane8 < half_lanes, own, v)

    def ext_sweep(mode, l, src, dst, size, reach):
        nt, origin = ext[l][2], ext[l][3]
        nx, ny, _ = dims[l]
        g = b[f"G{l}"]
        first = OWN - reach[0]
        rows = 8 * -(-(ny + sum(reach)) // 8)

        def some(i, count):
            for q in range(count):
                p = i + q
                new = stencil(mode, l, src, g, p, (p - 1, p + 1), first, rows, nt, True)
                for t, value in enumerate(new):
                    dst[p, t, pl.ds(first, rows), :] = value

        groups(origin - reach[0], origin + nx + reach[1], size, some)

    def spread_rows(q, v, j, c0, t):
        c, n = q[at(j, 0, t, OWN + c0)], q[at(j, 0, t, OWN + c0 + 1)]
        return c, 0.5 * (c + n)

    st, sg = b["stats"], [b[f"sums{a}"] for a in range(3)]

    def spread_sums(a):
        return [
            copy(st.at[a], sg[a].at[j], tuple(j if i == a else 0 for i in range(3)))
            for j in range(1, counts[a])
        ]

    def gather_sums(a, copies):
        wait(copies)
        total = st[a]
        for j in range(1, counts[a]):
            total = total + sg[a][j]
        if a < 2:
            st[a + 1] = total
        return total

    def fold(ref):
        def step(p, totals):
            totals = list(totals)
            for q in range(2):
                for k in range(nb0):
                    for t in range(nt0):
                        totals[(2 * k + t) % 4] += ref[at(2 * p + q, k, t)]
            return tuple(totals)

        t = lax.fori_loop(0, x0 // 2, step, (zero8,) * 4)
        return (t[0] + t[1]) + (t[2] + t[3])

    a1, b1, g1 = b["A1"], b["B1"], b["G1"]
    a2, b2, g2 = b["A2"], b["B2"], b["G2"]

    with jax.named_scope("clear"):

        def clear0(i, _):
            for ref in (u, a0, b0, d0):
                for t in range(nt0):
                    ref[i, t, pl.ds(0, OWN), :] = zero8
                    if ref is not d0:
                        ref[i, t, pl.ds(OWN + y0, OWN), :] = zero8
            return 0

        for t in range(nt0):
            b["rx"][t, pl.ds(0, OWN), :] = zero8

        lax.fori_loop(0, x0, clear0, 0)
        for l in (1, 2):
            ex, ey, tiles, _ = ext[l]
            refs = [b[f"{name}{l}"] for name in "GAB"]

            def clear(i, _, refs=refs, ey=ey, tiles=tiles):
                for ref in refs:
                    for k in range(ey // 8):
                        for t in range(tiles):
                            ref[at(i, k, t, 0)] = zero8
                return 0

            lax.fori_loop(0, ex, clear, 0)
            for side in range(2):
                for slot in range(b[f"hz{l}"].shape[1]):
                    for k in range(ey // 8):
                        b[f"hz{l}"][side, slot, pl.ds(8 * k, 8), :] = zero8
        for p in range(b["P2"].shape[0]):
            for k in range(ext[2][1] // 8):
                b["P2"][p, pl.ds(8 * k, 8), :] = zero8
    with jax.named_scope("loadu"):
        loads[0].wait()
        loads[1].wait()
    with jax.named_scope("packu"):

        def pack_some(i, count):
            for q in range(count):
                pack_z(b["zp"].at[0], i + q, u)

        groups(0, x0, 8, pack_some)
    with jax.named_scope("sumu"):
        st[0, 0] = fold(u)
    with jax.named_scope("barrier"):
        pl.semaphore_wait(barrier, len(offsets))
    send_x, send_y, send_z = exchange(0, u)
    moving = send_x() + send_y() + send_z()
    with jax.named_scope("sumf"):
        loads[2].wait()
        loads[3].wait()
        st[0, 1] = fold(f)
    sums = spread_sums(0)
    faces = b["yp"]
    moving = sweep(0, moving, u, a0, exchange(1, a0, faces.at[1]))
    gather_sums(0, sums)
    sums = spread_sums(1)
    moving = sweep(1, moving, a0, b0, exchange(2, b0, faces.at[0]))
    gather_sums(1, sums)
    sums = spread_sums(2)
    moving = sweep(2, moving, b0, d0, defect_exchange(3, d0), mode="defect")
    total = gather_sums(2, sums)
    mean_u = jnp.sum(total[0]) * (1.0 / cells)
    mean_f = jnp.sum(total[1]) * (1.0 / cells)

    o1, own1 = ext[1][3], pl.ds(OWN, y1)
    w0 = restrict_matrix(z0, LANES, z1)
    with jax.named_scope("restrict0"):
        restrict_planes(d0, None, 0, 0, nb0 + 1, nt0, b["T0"])
        multiply(b["T0"], g1, w0, 0, x1, 8, pl.ds(0, y1), o1, own1, mean_f)
    with jax.named_scope("step3"):

        def step3(i, count):
            for q in range(count):
                for t in range(nt0):
                    a0[i + q, t, own0, :] = b0[i + q, t, own0, :] + W * d0[i + q, t, own0, :]
            for q in range(count):
                pack_z(b["zp"].at[0], i + q, a0)

        groups(0, x0, 8, step3)
    wait(moving)

    with jax.named_scope("edges0"):
        lane = lax.broadcasted_iota(jnp.int32, (y0 + 8, LANES), 1)
        moved = pltpu.roll(b["rw"][...], 1, 1)
        rim = jnp.where(lane == last, moved, b["rz"][...])
        b["m"][...] = dot_split(rim, restrict_matrix(LANES, LANES, x1, last, 2))
        m, edge = b["m"], b["e"]

        def every_other(ref, n):
            v = 0.25 * (ref[pl.ds(OWN - 1, n, stride=2), :] + ref[pl.ds(OWN + 1, n, stride=2), :])
            return 0.25 * (v + 0.5 * ref[pl.ds(OWN, n, stride=2), :])

        rims = []
        for t in range(nt0):
            ry, rx = every_other(b["ry"].at[t], x1), every_other(b["rx"].at[t], y1)
            rims.append(jnp.concatenate([ry, rx], 0))
        edge[...] = dot_split(jnp.concatenate(rims, 1), w0)
        b["n"][...] = every_other(m, y1)
        g1[o1, 0, own1, :] = g1[o1, 0, own1, :] + edge[pl.ds(x1, y1), :]

        def finish(i, count):
            lane = lanes_of(y1)
            done = []
            for q in range(count):
                col = pltpu.roll(b["n"][...], turn(2 * LANES - (i + q)), 1)
                v = g1[i + q + o1, 0, own1, :] + jnp.where(lane == 0, col, 0.0)
                top = v[:8] + jnp.where(row8 == 0, edge[pl.ds(i + q, 1), :], 0.0)
                done.append((i + q + o1, OWN, top))
                done.append((i + q + o1, OWN + 8, v[8:]))
            for p, start, v in done:
                g1[p, 0, pl.ds(start, v.shape[0]), :] = v

        groups(0, x1, 16, finish)
    with jax.named_scope("pack1"):
        halo_pack1()
    moving = halo_send(1, g1.at[:, 0], x1, HALO1, HALO1)
    t1 = b["T1"]
    depth2 = (low_pairs, high_pairs)
    halo2 = []

    def between():
        wait(moving)
        send_x, send_y, send_z = exchange(4, a0)
        started = send_x() + send_y() + send_z()
        with jax.named_scope("unpack1"):
            halo_unpack1()
        with jax.named_scope("first1"):
            ext_sweep("first", 1, g1, b1, 13, (3, 4))
        with jax.named_scope("defect1"):
            ext_sweep("defect", 1, b1, a1, 19, (1, 0))
        with jax.named_scope("restrict1"):
            blocks1 = -(-(y1 + 1) // 8)
            restrict_planes(a1, o1 - 1, o1, OWN - 1, blocks1, 2, t1)
            w = restrict_matrix(2 * LANES, LANES // 2, z2, 2 * LANES - 1)
            none = jnp.zeros_like(w)
            w = jnp.concatenate([jnp.concatenate([w, none], 1), jnp.concatenate([none, w], 1)], 0)
            paired = []
            for half in range(2):
                for t in range(2):
                    v = [t1[2 * p + half, t] for p in range(pairs)]
                    paired.append(jnp.concatenate(v, 0))
            v = dot_split(jnp.concatenate(paired, 1), w).reshape(pairs, y2, LANES)
            b["P2"][pl.ds(low_pairs, pairs), pl.ds(OWN, y2), :] = v
        with jax.named_scope("pack2"):
            halo_pack2()
        halo2.extend(halo_send(2, b["P2"], pairs, depth2, HALO2))
        return started

    sweep(4, between, a0, b0)
    wait(halo2)
    with jax.named_scope("unpack2"):
        halo_unpack2()
    with jax.named_scope("sweeps2"):
        v, w2 = a2, b2
        reach = [(k + 2, k + 3) for k in range(COARSE_SWEEPS - 1)][::-1]
        ext_sweep("first", 2, g2, v, 27, reach[0])
        for k in range(1, COARSE_SWEEPS - 1):
            ext_sweep("relax", 2, v, w2, 27, reach[k])
            v, w2 = w2, v
    with jax.named_scope("prolong1"):
        o2 = ext[2][3]
        q1, v1 = b["Q1"], b["V1"]
        w = prolong_matrix(LANES, 2 * LANES, z1, True)
        multiply(v, q1, w, o2 - 2, x2 + 5, x2 + 5, pl.ds(0, ext[2][1]), 0, pl.ds(0, ext[2][1]))

        def spread1(i, count):
            for q in range(count):
                for t in range(2):
                    for c0 in range(-2, (y1 + 3) // 2, 8):
                        even, odd = spread_rows(q1, v1, i + q, c0, t)
                        v1[i + q, t, pl.ds(OWN + 2 * c0, 8, stride=2), :] = even
                        v1[i + q, t, pl.ds(OWN + 2 * c0 + 1, 8, stride=2), :] = odd

        groups(o2 - 2, o2 + x2 + 3, 7, spread1)

        def add1(i, count):
            for q in range(count):
                j = i + q
                rows = pl.ds(OWN - 3, 8 * -(-(y1 + 7) // 8))
                for t in range(2):
                    c, n = v1[j + o2, t, rows, :], v1[j + 1 + o2, t, rows, :]
                    even, odd = 2 * j + o1, 2 * j + o1 + 1
                    b1[even, t, rows, :] = b1[even, t, rows, :] + c
                    b1[odd, t, rows, :] = b1[odd, t, rows, :] + 0.5 * (c + n)

        groups(-2, x2 + 2, 4, add1)
    with jax.named_scope("post1"):
        ext_sweep("relax", 1, b1, a1, 19, (2, 3))
        ext_sweep("relax", 1, a1, b1, 18, (1, 2))
    keep = 1.0 - relax_weight
    coarse = [b[name] for name in ("CA", "CB", "CC")]
    fine = [u, d0, a0]

    def spread(a, bb, c):
        be, bo = bb[-1] + bb[1], bb[0] + bb[1]
        ce, co = c[0] + c[0] + (c[-1] + c[1]), c[0] + c[1]
        e0 = a[0] + (bb[0] + 0.5 * be) + ce
        o0 = 0.5 * ((a[0] + a[1]) + (c[-1] + c[2])) + (bo + 1.5 * co)
        return e0, o0, (bb[0] + ce, 0.5 * bo + 2.0 * co), (c[0], 0.5 * co)

    with jax.named_scope("tailz"):
        shift = mean_u + 4.0 * W * mean_f
        w = hat_matrices(2 * LANES, z0)
        chunk, rows = x1 + 3, pl.ds(OWN - 1, y1 + 8)

        def tail_z(k, _):
            i = k * chunk
            v = dot_split(planes_of(b1, i + o1 - 1, chunk, rows), w)
            for t in range(nt0):
                z = [v[:, z0 * n + LANES * t : z0 * n + LANES * t + LANES] for n in range(3)]
                ca = keep**2 * z[0] + (2.0 * keep * W) * z[1] + W**2 * z[2] - shift
                cb = (2.0 * keep * W) * z[0] + (2.0 * W**2) * z[1]
                for ref, value in zip(coarse, (ca, cb, W**2 * z[0])):
                    ref[pl.ds(i, chunk), t, rows, :] = value.reshape(chunk, -1, LANES)
            return 0

        tail_z(0, 0)
    with jax.named_scope("taily"):

        def tail_y(i, count):
            for q in range(count):
                for t in range(nt0):
                    near = [
                        {d: ref[i + q, t, pl.ds(OWN + d, y1), :] for d in (-1, 0, 1, 2)}
                        for ref in coarse
                    ]
                    e0, o0, one, two = spread(*near)
                    for ref, even, odd in ((fine[0], e0, o0), (fine[1], *one), (fine[2], *two)):
                        ref[i + q, t, pl.ds(0, y1, stride=2), :] = even
                        ref[i + q, t, pl.ds(1, y1, stride=2), :] = odd

        groups(0, x1 + 3, 5, tail_y)
    with jax.named_scope("tailx"):
        rows0 = pl.ds(0, y0)

        def tail_x(i, count):
            for q in range(count):
                j = i + q
                for t in range(nt0):
                    near = [
                        {d: ref[j + 1 + d, t, rows0, :] for d in (-1, 0, 1, 2)} for ref in fine
                    ]
                    e0, o0, _, _ = spread(*near)
                    lanes = pl.ds(LANES * t, LANES)
                    out[2 * j, :, lanes] = b0[2 * j, t, own0, :] + e0
                    out[2 * j + 1, :, lanes] = b0[2 * j + 1, t, own0, :] + o0

        groups(0, x1, 4, tail_x)


def solution(mesh):
    counts = tuple(mesh.shape[a] for a in AXES)

    def shards(right_side, initial_guess):
        shape = right_side.shape
        dims = tuple(tuple(n >> l for n in shape) for l in range(3))
        cells = float(right_side.size)
        for n in counts:
            cells *= n
        bufs = buffers(dims, counts)
        messages = 2 * 8 + 2 * 6 + 9 + 2 * 26 + sum(counts) - 3
        return pl.pallas_call(
            functools.partial(kernel, dims, counts, tuple(bufs), cells),
            out_shape=jax.ShapeDtypeStruct(shape, jnp.float32),
            in_specs=[pl.BlockSpec(memory_space=pl.ANY)] * 2,
            out_specs=pl.BlockSpec(memory_space=pltpu.VMEM),
            scratch_shapes=list(bufs.values())
            + [pltpu.SemaphoreType.DMA((n,)) for n in (messages, messages, 4)],
            compiler_params=pltpu.CompilerParams(
                collective_id=0, has_side_effects=True, vmem_limit_bytes=56 * 1024 * 1024
            ),
        )(initial_guess, right_side)

    placed = (P(*AXES), P(*AXES))
    return jax.shard_map(
        shards, mesh=mesh, in_specs=placed, out_specs=P(*AXES), check_vma=False
    )
```
